32 devices in a mesh: seq: 8 (over z, core), head: 4 (over y, x).
Axes of the slice: x: 2, y: 2, z: 4, core: 2. Of those that a mesh axis runs over, the one named last changes fastest.
Arguments:
- grid_state: bfloat16 [65536, 1024], P('seq', 'head'), may hold values from -6 to 6
- encode_index: int32 [128, 8], P('seq'), may hold values from 0 to 511, as said below
- encode_weights: bfloat16 [128, 8, 128, 128], P('seq'), may hold values from -0.1875 to 0.1875
- first_gain: float32 [1024], replicated, may hold values from 0.1 to 1.9
- project_in: bfloat16 [1024, 3, 1024], P(None, None, 'head'), may hold values from -8 to 8
- project_out: bfloat16 [1024, 1024], P('head'), may hold values from -0.25 to 0.25
- second_gain: float32 [1024], replicated, may hold values from 0.1 to 1.9
- expand_weights: bfloat16 [1024, 4096], P(None, 'head'), may hold values from -0.1875 to 0.1875
- shrink_weights: bfloat16 [4096, 1024], P('head'), may hold values from -0.125 to 0.125
- decode_index: int32 [512, 2], P('seq'), may hold values from 0 to 127, as said below
- decode_weights: bfloat16 [512, 2, 128, 128], P('seq'), may hold values from -0.375 to 0.375
- output_gain: float32 [1024], P('head'), may hold values from 0.1 to 1.9
Outputs:
- grid_output: bfloat16 [65536, 1024], P('seq', 'head')
The draws below stay inside these ranges and needn't reach their ends.
Inputs may be any that keep to these rules, and one draw needn't show every extreme that they name: `encode_index`: for a mesh block of band b (blocks b * 16 onward), every entry lies in b * 64 - 2048 / 128 to (b + 1) * 64 + 2048 / 128 - 1. `decode_index`: for a grid block of band b (blocks b * 64 onward), every entry lies in b * 16 - 2048 / 256 to (b + 1) * 16 + 2048 / 256 - 1, with the division rounded down.
All inputs are finite; a program needn't handle non-finite values.
Results may differ from the reference program's by a relative error of at most 0.012.
Values may be sent and summed in bfloat16 or wider, within the bound.
A program may use at most 128 MiB of HBM per device.

```python
import jax
import jax.numpy as jnp
from jax import lax

D = 1024
HEADS = 16
MLP = 4096
HEAD_DIM = 64
WINDOW = 1120
M_DEV = 2048
G_DEV = 8192
BLOCK = 128
SLOTS_IN = 8
SLOTS_OUT = 2
GRID = 65536
MESH_BLOCKS = 128
GRID_BLOCKS = 512


def band_table(key, row_count, rows_band, rim_blocks, own_blocks, total_blocks, slot_count):
    row_iota = jnp.arange(row_count, dtype=jnp.int32)
    band_number = row_iota // rows_band
    lowest = jnp.maximum(band_number * own_blocks - rim_blocks, 0)
    highest = jnp.minimum((band_number + 1) * own_blocks + rim_blocks, total_blocks)
    drawn = jax.random.randint(key, (row_count, slot_count), lowest[:, None], highest[:, None])
    within = row_iota % rows_band
    drawn = drawn.at[:, 0].set(jnp.where(within == 0, lowest, drawn[:, 0]))
    drawn = drawn.at[:, slot_count - 1].set(jnp.where(within == rows_band - 1, highest - 1, drawn[:, slot_count - 1]))
    return drawn.astype(jnp.int32)


def draw_encode_index(key, part):
    mesh_band = M_DEV // BLOCK
    return band_table(jax.random.fold_in(key, 11), MESH_BLOCKS, mesh_band, mesh_band, G_DEV // BLOCK, GRID_BLOCKS, SLOTS_IN)


def draw_decode_index(key, part):
    mesh_band = M_DEV // BLOCK
    return band_table(jax.random.fold_in(key, 13), GRID_BLOCKS, G_DEV // BLOCK, mesh_band // 2, mesh_band, MESH_BLOCKS, SLOTS_OUT)


def draw_project_in(key, part):
    matrix = jax.random.normal(jax.random.fold_in(key, 17), (D, 3, D), jnp.float32) * D ** (-0.5)
    return jnp.clip(matrix, -8.0, 8.0).astype(jnp.bfloat16)


def strengthened(array, key, source, target, parts, factor):
    owner, partner = [(jnp.arange(array.shape[dim]) // (array.shape[dim] // parts)).reshape([-1 if axis == dim else 1 for axis in range(array.ndim)]) for dim in (source, target)]
    chosen = jax.random.permutation(key, parts)[partner]
    strong = (owner == chosen) | (owner == (partner + parts // 2) % parts)
    return jnp.where(strong, factor * array, array)


def level_of(stream_key, shape, pieces, least, high):
    def one(dim, blocks):
        steps = jax.random.uniform(jax.random.fold_in(jax.random.fold_in(stream_key, 6), dim), (blocks,), jnp.float32, least / len(pieces), high / len(pieces))
        return jnp.repeat(jnp.exp(steps), shape[dim] // blocks).reshape((-1,) + (1,) * (len(shape) - dim - 1))

    factor_of = one(*pieces[0])
    for cut in pieces[1:]:
        factor_of = factor_of * one(*cut)
    return factor_of


def bell_draw(key, extent, scale, limit, split=(), held_as=jnp.bfloat16):
    level = level_of(key, extent, split, -0.22, 0.18) if split else 1.0
    result = jax.random.normal(key, extent, jnp.float32) * scale * level
    return jnp.minimum(jnp.maximum(result, -limit), limit).astype(held_as)


def heavy_noise(own_key, shape, scale, bound, cuts, heavy, kind=jnp.bfloat16):
    result = scale * jax.random.normal(own_key, shape, jnp.float32)
    if cuts:
        result = result * level_of(own_key, shape, cuts, -0.22, 0.18)
    return jnp.clip(strengthened(result, jax.random.fold_in(own_key, 3), *heavy), -bound, bound).astype(kind)


def setup_inputs(seed: int = 0) -> dict:
    key_of = jax.random.split(jax.random.key(seed), 13)
    return {
        "grid_state": bell_draw(key_of[0], (GRID, D), 1.0, 6.0, ((0, 8), (1, 4))),
        "encode_index": draw_encode_index(jax.random.fold_in(key_of[12], 71), 0),
        "encode_weights": bell_draw(key_of[2], (MESH_BLOCKS, SLOTS_IN, BLOCK, BLOCK), (SLOTS_IN * BLOCK) ** -0.5, 0.1875, ((0, 8),)),
        "first_gain": jnp.clip(1.0 + 0.18 * jax.random.normal(key_of[3], (D,), jnp.float32), 0.1, 1.9),
        "project_in": draw_project_in(jax.random.fold_in(key_of[12], 71), 0),
        "project_out": heavy_noise(key_of[5], (D, D), D ** -0.5, 0.25, ((0, 4),), (0, 1, 4, 2.0)),
        "second_gain": jnp.clip(1.0 + 0.18 * jax.random.normal(key_of[6], (D,), jnp.float32), 0.1, 1.9),
        "expand_weights": bell_draw(key_of[7], (D, MLP), D ** -0.5, 0.1875, ((1, 4),)),
        "shrink_weights": heavy_noise(key_of[8], (MLP, D), MLP ** -0.5, 0.125, ((0, 4),), (0, 1, 4, 2.0)),
        "decode_index": draw_decode_index(jax.random.fold_in(key_of[12], 71), 0),
        "decode_weights": bell_draw(key_of[10], (GRID_BLOCKS, SLOTS_OUT, BLOCK, BLOCK), (SLOTS_OUT * BLOCK) ** -0.5, 0.375, ((0, 8),)),
        "output_gain": jnp.clip(1.0 + 0.18 * jax.random.normal(key_of[11], (D,), jnp.float32), 0.1, 1.9),
    }


EPSILON = 1e-05

def settle(values):
    return lax.optimization_barrier(values)

def layer_norm(values, scales):
    average = lax.optimization_barrier(jnp.mean(values, axis=1, keepdims=True))
    centred = values - average
    spread = lax.optimization_barrier(jnp.mean(centred * centred, axis=1, keepdims=True))
    return centred * lax.rsqrt(spread + EPSILON) * scales

def interpolate(source, index_table, weight_table):
    columns = source.shape[1]
    blocks = source.reshape(-1, BLOCK, columns)

    def one_block(pair):
        position, weight_block = pair
        picked = jnp.take(blocks, position, axis=0).astype(jnp.float32)
        return jnp.einsum('kij,kjc->ic', weight_block.astype(jnp.float32), picked, precision=lax.Precision.HIGHEST)
    return lax.map(one_block, (index_table, weight_table)).reshape(-1, columns)

def window_mask(query_rows, key_count, key_anchor, total_rows):
    query_iota = lax.broadcasted_iota(jnp.int32, (query_rows, key_count), 0)
    key_iota = lax.broadcasted_iota(jnp.int32, (query_rows, key_count), 1)
    distance = key_iota - query_iota
    global_key = key_anchor + key_iota
    return (distance >= 0) & (distance <= 2 * WINDOW) & (global_key >= 0) & (global_key < total_rows)

def softmax_values(scores, allowed, value_block):
    masked = jnp.where(allowed[None], scores, -1e+30)
    highest = lax.optimization_barrier(jnp.max(masked, axis=2, keepdims=True))
    powers = jnp.where(allowed[None], jnp.exp(masked - highest), 0.0)
    probs = settle((powers / lax.optimization_barrier(jnp.sum(powers, axis=2, keepdims=True))).astype(jnp.bfloat16))
    context = jnp.einsum('hqk,khd->qhd', probs.astype(jnp.float32), value_block, precision=lax.Precision.HIGHEST)
    return context.astype(jnp.bfloat16)

def attention(queries, keys, values):
    total_rows = queries.shape[0]
    query_rows = min(512, M_DEV)
    key_count = query_rows + 2 * WINDOW
    padding = ((WINDOW, WINDOW), (0, 0), (0, 0))
    keys_wide = jnp.pad(keys, padding)
    values_wide = jnp.pad(values, padding)

    def attend(first_row):
        query_block = lax.dynamic_slice_in_dim(queries, first_row, query_rows, 0).astype(jnp.float32)
        key_block = lax.dynamic_slice_in_dim(keys_wide, first_row, key_count, 0).astype(jnp.float32)
        value_block = lax.dynamic_slice_in_dim(values_wide, first_row, key_count, 0).astype(jnp.float32)
        scores = jnp.einsum('qhd,khd->hqk', query_block, key_block, precision=lax.Precision.HIGHEST) * HEAD_DIM ** (-0.5)
        allowed = window_mask(query_rows, key_count, first_row - WINDOW, total_rows)
        return softmax_values(scores, allowed, value_block)
    starts = jnp.arange(total_rows // query_rows, dtype=jnp.int32) * query_rows
    return lax.map(attend, starts).reshape(total_rows, HEADS * HEAD_DIM)

def reference(grid_state, encode_index, encode_weights, first_gain, project_in, project_out, second_gain, expand_weights, shrink_weights, decode_index, decode_weights, output_gain):
    mesh_start = settle(interpolate(grid_state, encode_index, encode_weights).astype(jnp.bfloat16))
    first_norm = layer_norm(mesh_start.astype(jnp.float32), first_gain).astype(jnp.bfloat16)
    heads_shape = (mesh_start.shape[0], HEADS, HEAD_DIM)
    queries = settle(jnp.dot(first_norm, project_in[:, 0, :], preferred_element_type=jnp.float32).astype(jnp.bfloat16)).reshape(heads_shape)
    keys = settle(jnp.dot(first_norm, project_in[:, 1, :], preferred_element_type=jnp.float32).astype(jnp.bfloat16)).reshape(heads_shape)
    values = settle(jnp.dot(first_norm, project_in[:, 2, :], preferred_element_type=jnp.float32).astype(jnp.bfloat16)).reshape(heads_shape)
    context = attention(queries, keys, values)
    attended = jnp.dot(context, project_out, preferred_element_type=jnp.float32)
    mesh_middle = settle((mesh_start.astype(jnp.float32) + attended).astype(jnp.bfloat16))
    second_norm = layer_norm(mesh_middle.astype(jnp.float32), second_gain).astype(jnp.bfloat16)
    hidden = jax.nn.gelu(jnp.dot(second_norm, expand_weights, preferred_element_type=jnp.float32)).astype(jnp.bfloat16)
    shrunk = jnp.dot(hidden, shrink_weights, preferred_element_type=jnp.float32)
    mesh_end = settle((mesh_middle.astype(jnp.float32) + shrunk).astype(jnp.bfloat16))
    back = interpolate(mesh_end, decode_index, decode_weights)
    average = lax.optimization_barrier(jnp.sum(back, axis=1, keepdims=True)) / D
    squares = lax.optimization_barrier(jnp.sum(back * back, axis=1, keepdims=True)) / D
    normed = (back - average) * lax.rsqrt(squares - average * average + EPSILON) * output_gain
    return (grid_state.astype(jnp.float32) + normed).astype(jnp.bfloat16)
```

```python
import functools

import jax
import jax.numpy as jnp
from jax import lax
from jax.experimental import pallas as pl
from jax.experimental.pallas import tpu as pltpu
from jax.sharding import PartitionSpec as P

D = 1024
HEAD_DIM = 64
WINDOW = 1120
EPSILON = 1e-05
NEGATIVE = -1e30
Q_TILE = 256
K_CHUNK = 512
F32 = jnp.float32
BF16 = jnp.bfloat16
MIB = 1024 * 1024


def params(mib=48, dims=None):
    return pltpu.CompilerParams(vmem_limit_bytes=mib * MIB, dimension_semantics=dims)


def cost(flops, moved):
    return pl.CostEstimate(flops=int(flops), bytes_accessed=int(moved), transcendentals=0)


def rims(cells, width):
    count = lax.axis_size("seq")
    up = [(i, i + 1) for i in range(count - 1)]
    down = [(i + 1, i) for i in range(count - 1)]
    lower = lax.ppermute(cells[cells.shape[0] - width :], "seq", up)
    upper = lax.ppermute(cells[:width], "seq", down)
    return lower, upper


def flipped(value, bit):
    count = lax.axis_size("head")
    return lax.ppermute(value, "head", [(i, i ^ bit) for i in range(count)])


def load_wide(parts, wide, sems):
    copies = []
    at = 0
    for number, part in enumerate(parts):
        rows = part.shape[0]
        copies.append(pltpu.make_async_copy(part, wide.at[pl.ds(at, rows)], sems.at[number]))
        at += rows
    for copy in copies:
        copy.start()
    for copy in copies:
        copy.wait()


def gathered_dot(table, weights, wide, block, local, slots):
    rows = weights.shape[2]
    picked = []
    for k in range(slots):
        at = pl.multiple_of(table[block * slots + k] * rows, rows)
        picked.append(wide[pl.ds(at, rows), :])
    left = jnp.concatenate([weights[local, k] for k in range(slots)], axis=1)
    return left, jnp.concatenate(picked, axis=0)


def reach(src, dst, send, recv, **target):
    return pltpu.make_async_remote_copy(
        src_ref=src,
        dst_ref=dst,
        send_sem=send,
        recv_sem=recv,
        device_id=target,
        device_id_type=pl.DeviceIdType.MESH,
    )


def greet(bands, heads):
    band = lax.axis_index("seq")
    head = lax.axis_index("head")
    barrier = pltpu.get_barrier_semaphore()
    kind = pl.DeviceIdType.MESH
    for j in range(1, heads):
        pl.semaphore_signal(barrier, inc=1, device_id={"head": head ^ j}, device_id_type=kind)

    @pl.when(band > 0)
    def _():
        pl.semaphore_signal(barrier, inc=1, device_id={"seq": band - 1}, device_id_type=kind)

    @pl.when(band < bands - 1)
    def _():
        pl.semaphore_signal(barrier, inc=1, device_id={"seq": band + 1}, device_id_type=kind)

    ends = (band > 0).astype(jnp.int32) + (band < bands - 1).astype(jnp.int32)
    pl.semaphore_wait(barrier, heads - 1 + ends)


def front_kernel(bands, heads, rim_rows, *refs):
    table, state, blend, gain, weight_q, weight_kv = refs[:6]
    out_q, out_kv, out_low, out_high, out_start = refs[6:11]
    wide, weights, held, q_weights, kv_weights = refs[11:16]
    loads, rim_send, rim_recv, piece_send, piece_recv, kv_send, kv_recv = refs[16:]
    band = lax.axis_index("seq")
    head = lax.axis_index("head")
    blocks, slots, rows, _ = weights.shape
    grid_blocks, _, columns = state.shape
    mesh_rows = blocks * rows
    margin = (wide.shape[0] - grid_blocks) // 2
    chunk = 256
    chunks = mesh_rows // chunk
    has_low = band > 0
    has_high = band < bands - 1
    lower = lax.max(band - 1, 0)
    upper = lax.min(band + 1, bands - 1)

    local = [
        pltpu.make_async_copy(state, wide.at[pl.ds(margin, grid_blocks)], loads.at[0]),
        pltpu.make_async_copy(blend, weights, loads.at[1]),
        pltpu.make_async_copy(weight_q, q_weights, loads.at[2]),
        pltpu.make_async_copy(weight_kv, kv_weights, loads.at[3]),
    ]
    for copy in local:
        copy.start()
    greet(bands, heads)

    down = reach(
        state.at[pl.ds(0, margin)],
        wide.at[pl.ds(margin + grid_blocks, margin)],
        rim_send.at[0],
        rim_recv.at[1],
        seq=lower,
    )
    up = reach(
        state.at[pl.ds(grid_blocks - margin, margin)],
        wide.at[pl.ds(0, margin)],
        rim_send.at[1],
        rim_recv.at[0],
        seq=upper,
    )
    pl.when(has_low)(down.start)
    pl.when(has_high)(up.start)

    @pl.when(jnp.logical_not(has_low))
    def _():
        out_low[...] = jnp.zeros(out_low.shape, BF16)

    @pl.when(jnp.logical_not(has_high))
    def _():
        out_high[...] = jnp.zeros(out_high.shape, BF16)

    for copy in local:
        copy.wait()
    pl.when(has_low)(up.wait_recv)
    pl.when(has_high)(down.wait_recv)

    def place(step):
        number = jnp.where(band % 2 == 0, step, chunks - 1 - step)
        return number, pl.ds(pl.multiple_of(number * chunk, chunk), chunk)

    def piece(step, owner, partner):
        _, here = place(step)
        source = 0 if owner == partner else owner ^ partner
        return reach(
            held.at[source, here],
            held.at[owner, here],
            piece_send.at[owner, step],
            piece_recv.at[owner, step],
            head=head ^ partner,
        )

    def encode(step):
        number, _ = place(step)
        for part in range(chunk // rows):
            block = number * (chunk // rows) + part
            left = jnp.concatenate([weights[block, k] for k in range(slots)], axis=1)
            right = jnp.concatenate([wide[table[block * slots + k]] for k in range(slots)], axis=0)
            at = pl.multiple_of(number * chunk + part * rows, rows)
            held[0, pl.ds(at, rows), :] = jnp.dot(
                left, right, preferred_element_type=F32
            ).astype(BF16)

    def project(step):
        _, here = place(step)
        values = [held[j, here, :].astype(F32) for j in range(heads)]
        average = sum(jnp.sum(v, axis=1, keepdims=True) for v in values) / D
        centred = [v - average for v in values]
        spread = sum(jnp.sum(c * c, axis=1, keepdims=True) for c in centred) / D
        scale = lax.rsqrt(spread + EPSILON)
        queries, others = 0.0, 0.0
        for j in range(heads):
            owner = head ^ j
            normed = (centred[j] * scale * gain[owner]).astype(BF16)
            queries += jnp.dot(normed, q_weights[owner], preferred_element_type=F32)
            others += jnp.dot(normed, kv_weights[owner], preferred_element_type=F32)
        out_q[here, :] = (queries.astype(BF16).astype(F32) * HEAD_DIM ** (-0.5)).astype(BF16)
        out_kv[here, :] = others.astype(BF16)

    full, rest = divmod(rim_rows, chunk)
    first = mesh_rows - rim_rows

    def rim_copies(step):
        number, here = place(step)
        start = pl.multiple_of(number * chunk, chunk)
        made = []
        whole = jnp.logical_and(has_low, number < full)
        source = out_kv.at[here]
        target = out_high.at[pl.ds(pl.multiple_of(jnp.minimum(start, (full - 1) * chunk), chunk), chunk)]
        made.append((whole, reach(source, target, kv_send.at[0, step], kv_recv.at[0, number], seq=lower)))
        whole = jnp.logical_and(has_high, number >= chunks - full)
        target = out_low.at[pl.ds(pl.multiple_of(jnp.maximum(start - first, rest), 16), chunk)]
        made.append((whole, reach(source, target, kv_send.at[1, step], kv_recv.at[1, number], seq=upper)))
        if rest:
            part = jnp.logical_and(has_low, number == full)
            source = out_kv.at[pl.ds(full * chunk, rest)]
            target = out_high.at[pl.ds(full * chunk, rest)]
            made.append((part, reach(source, target, kv_send.at[0, step], kv_recv.at[0, number], seq=lower)))
            part = jnp.logical_and(has_high, number == chunks - full - 1)
            source = out_kv.at[pl.ds(first, rest)]
            target = out_low.at[pl.ds(0, rest)]
            made.append((part, reach(source, target, kv_send.at[1, step], kv_recv.at[1, number], seq=upper)))
        return made

    def arrival(way, number, size, at):
        into = (out_high if way == 0 else out_low).at[pl.ds(at, size)]
        spare = kv_send.at[way, 0]
        return reach(into, into, spare, kv_recv.at[way, number], seq=upper if way == 0 else lower)

    relay = heads == 4

    def diagonal(step):
        return piece(step, 3, 2) if step % 2 == 0 else piece(step, 3, 1)

    def relayed(step):
        return 1 if step % 2 == 0 else 2

    for step in range(chunks + 2):
        if step < chunks:
            encode(step)
            for j in (range(1, 3) if relay else range(1, heads)):
                piece(step, j, j).start()
        if relay and 1 <= step <= chunks:
            piece(step - 1, relayed(step - 1), relayed(step - 1)).wait_recv()
            diagonal(step - 1).start()
        if step >= 2:
            old = step - 2
            for j in range(1, heads):
                if not (relay and j == relayed(old)):
                    piece(old, j, j).wait_recv()
            project(old)
            for here, copy in rim_copies(old):
                pl.when(here)(copy.start)

    share = out_start.shape[1]
    mine = pl.ds(pl.multiple_of(head * share, share), share)
    for j in range(heads):
        out_start[head ^ j] = held[j, mine, :]

    pl.when(has_low)(down.wait_send)
    pl.when(has_high)(up.wait_send)
    for step in range(chunks):
        for j in (range(1, 3) if relay else range(1, heads)):
            piece(step, j, j).wait_send()
        if relay:
            diagonal(step).wait_send()
        for here, copy in rim_copies(step):
            pl.when(here)(copy.wait_send)

    for number in range(full):
        pl.when(has_high)(arrival(0, number, chunk, number * chunk).wait_recv)
        other = chunks - full + number
        pl.when(has_low)(arrival(1, other, chunk, rest + number * chunk).wait_recv)
    if rest:
        pl.when(has_high)(arrival(0, full, rest, full * chunk).wait_recv)
        pl.when(has_low)(arrival(1, chunks - full - 1, rest, 0).wait_recv)


def front(bands, heads, table, state, blend, gain, weight_q, weight_kv):
    blocks, slots, rows, _ = blend.shape
    grid_rows, columns = state.shape
    grid_blocks = grid_rows // rows
    state = state.reshape(grid_blocks, rows, columns)
    mesh_rows = blocks * rows
    rim_rows = min(mesh_rows, WINDOW)
    chunks = mesh_rows // 256
    vmem = pl.BlockSpec(memory_space=pltpu.VMEM)
    hbm = pl.BlockSpec(memory_space=pl.ANY)
    shape = lambda *sizes: jax.ShapeDtypeStruct(sizes, BF16)
    dma = pltpu.SemaphoreType.DMA
    return pl.pallas_call(
        functools.partial(front_kernel, bands, heads, rim_rows),
        out_shape=[
            shape(mesh_rows, columns),
            shape(mesh_rows, 2 * columns),
            shape(rim_rows, 2 * columns),
            shape(rim_rows, 2 * columns),
            shape(heads, mesh_rows // heads, columns),
        ],
        in_specs=[pl.BlockSpec(memory_space=pltpu.SMEM), hbm, hbm, vmem, hbm, hbm],
        out_specs=[vmem] * 5,
        scratch_shapes=[
            pltpu.VMEM((grid_blocks + 2 * blocks, rows, columns), BF16),
            pltpu.VMEM(blend.shape, BF16),
            pltpu.VMEM((heads, mesh_rows, columns), BF16),
            pltpu.VMEM(weight_q.shape, BF16),
            pltpu.VMEM(weight_kv.shape, BF16),
            dma((4,)),
            dma((2,)),
            dma((2,)),
            dma((heads, chunks)),
            dma((heads, chunks)),
            dma((2, chunks)),
            dma((2, chunks)),
        ],
        compiler_params=pltpu.CompilerParams(
            vmem_limit_bytes=60 * MIB, collective_id=0, has_side_effects=True
        ),
        cost_estimate=cost(6 * mesh_rows * D * columns * 20, grid_rows * columns * 4),
        name="front",
    )(table, state, blend, gain, weight_q, weight_kv)


def attend_kernel(total, place, queries, low, own, high, out, wide, scores, masks):
    tile_number = pl.program_id(1)
    rim = low.shape[0]
    rows = own.shape[0]
    width = scores.shape[2]
    chunks = width // K_CHUNK

    @pl.when(tile_number == 0)
    def _():
        for a in range(2):
            lanes = slice(128 * a, 128 * (a + 1))
            wide[a, 0:rim, :] = low[:, lanes]
            wide[a, rim : rim + rows, :] = own[:, lanes]
            wide[a, rim + rows : 2 * rim + rows, :] = high[:, lanes]
            end = wide.shape[1] - (2 * rim + rows)
            wide[a, 2 * rim + rows :, :] = jnp.zeros((end, 128), BF16)
        q_iota = lax.broadcasted_iota(jnp.int32, (Q_TILE, K_CHUNK), 0)
        k_iota = lax.broadcasted_iota(jnp.int32, (Q_TILE, K_CHUNK), 1)
        for n, c in enumerate((0, chunks - 1)):
            distance = k_iota + c * K_CHUNK - q_iota
            allowed = (distance >= 0) & (distance <= 2 * WINDOW)
            masks[n] = jnp.where(allowed, 0.0, NEGATIVE)

    start = pl.multiple_of(tile_number * Q_TILE, Q_TILE)
    anchor = place[0] - WINDOW + start
    lane = lax.broadcasted_iota(jnp.int32, (Q_TILE, 128), 1)
    peaks = []
    for a in range(2):
        here = (lane < HEAD_DIM) if a == 0 else (lane >= HEAD_DIM)
        query = jnp.where(here, queries[...].astype(F32), 0.0).astype(BF16)
        peak = None
        for c in range(chunks):
            key = wide[a, pl.ds(start + c * K_CHUNK, K_CHUNK), :]
            score = lax.dot_general(
                query, key, (((1,), (1,)), ((), ())), preferred_element_type=F32
            )
            number = anchor + c * K_CHUNK + lax.broadcasted_iota(jnp.int32, (1, K_CHUNK), 1)
            score += jnp.where((number >= 0) & (number < total), 0.0, NEGATIVE)
            if c == 0:
                score += masks[0]
            if c == chunks - 1:
                score += masks[1]
            scores[a, :, c * K_CHUNK : (c + 1) * K_CHUNK] = score
            for part in range(K_CHUNK // 128):
                piece = score[:, part * 128 : (part + 1) * 128]
                peak = piece if peak is None else jnp.maximum(peak, piece)
        peaks.append(jnp.max(peak, axis=1, keepdims=True))
    results = []
    for a in range(2):
        gathered, weight = 0.0, 0.0
        for c in range(chunks):
            power = jnp.exp(scores[a, :, c * K_CHUNK : (c + 1) * K_CHUNK] - peaks[a])
            for part in range(K_CHUNK // 128):
                weight += power[:, part * 128 : (part + 1) * 128]
            value = wide[a, pl.ds(start + c * K_CHUNK, K_CHUNK), :]
            gathered += jnp.dot(power.astype(BF16), value, preferred_element_type=F32)
        results.append(gathered / jnp.sum(weight, axis=1, keepdims=True))
    out[...] = jnp.concatenate(
        [results[0][:, HEAD_DIM:], results[1][:, :HEAD_DIM]], axis=1
    ).astype(BF16)


def attend(place, total, queries, low, own, high):
    rows, columns = queries.shape
    rim = low.shape[0]
    width = -(-(Q_TILE + 2 * WINDOW) // K_CHUNK) * K_CHUNK
    wide_rows = rows - Q_TILE + width
    return pl.pallas_call(
        functools.partial(attend_kernel, total),
        out_shape=jax.ShapeDtypeStruct((rows, columns), BF16),
        grid_spec=pltpu.PrefetchScalarGridSpec(
            num_scalar_prefetch=1,
            grid=(columns // 128, rows // Q_TILE),
            in_specs=[
                pl.BlockSpec((Q_TILE, 128), lambda g, i, t: (i, g)),
                pl.BlockSpec((rim, 256), lambda g, i, t: (0, g)),
                pl.BlockSpec((rows, 256), lambda g, i, t: (0, g)),
                pl.BlockSpec((rim, 256), lambda g, i, t: (0, g)),
            ],
            out_specs=pl.BlockSpec((Q_TILE, 128), lambda g, i, t: (i, g)),
            scratch_shapes=[
                pltpu.VMEM((2, wide_rows, 128), BF16),
                pltpu.VMEM((2, Q_TILE, width), F32),
                pltpu.VMEM((2, Q_TILE, K_CHUNK), F32),
            ],
        ),
        compiler_params=params(60, ("arbitrary", "arbitrary")),
        cost_estimate=cost(16 * rows * width * columns, rows * columns * 8),
        name="attend",
    )(place, queries, low, own, high)


def feed_kernel(plan, units, *refs):
    context, start, gain, project_out = refs[:4]
    sources = refs[4:-6]
    out, normed, total, expand, shrink, sems = refs[-6:]
    width = context.shape[1]

    def copies(number):
        slot = number % 2
        made = []
        for source, rows, lanes, kind, at, to in plan[number]:
            buffer = expand if kind == "expand" else shrink
            taken = sources[source].at[pl.ds(rows[0], rows[1]), pl.ds(lanes[0], lanes[1])]
            placed = buffer.at[slot, pl.ds(at, rows[1]), pl.ds(to, lanes[1])]
            made.append(pltpu.make_async_copy(taken, placed, sems.at[slot, len(made)]))
        return made

    waiting = copies(0)
    for copy in waiting:
        copy.start()
    attended = jnp.dot(context[...], project_out[...], preferred_element_type=F32)
    begun = jnp.concatenate([start[j] for j in range(start.shape[0])], axis=1)
    middle = (begun.astype(F32) + attended).astype(BF16).astype(F32)
    total[...] = middle
    average = jnp.mean(middle, axis=1, keepdims=True)
    centred = middle - average
    spread = jnp.mean(centred * centred, axis=1, keepdims=True)
    normed[...] = (centred * lax.rsqrt(spread + EPSILON) * gain[...]).astype(BF16)
    for number in range(len(plan)):
        for copy in waiting:
            copy.wait()
        if number + 1 < len(plan):
            waiting = copies(number + 1)
            for copy in waiting:
                copy.start()
        slot = number % 2
        wide = jnp.dot(normed[...], expand[slot], preferred_element_type=F32)
        hidden = jax.nn.gelu(wide).astype(BF16)
        total[...] += jnp.dot(hidden, shrink[slot], preferred_element_type=F32)
    out[...] = total[...].astype(BF16)


def whole_entry(source, base, units, width):
    cuts = width // units
    entry = [(source[0], (source[1], width), (0, units), "expand", 0, 0)]
    for c in range(cuts):
        entry.append((base[0], (base[1] + c * units, units), (0, units), "shrink", 0, c * units))
    return entry


def feed(context, start, gain, project_out, expand, shrink, packs):
    rows, width = context.shape
    units = expand.shape[1] // 2
    sources = [expand, shrink]
    plan = []
    for half in range(2):
        plan.append(
            [
                (0, (0, width), (half * units, units), "expand", 0, 0),
                (1, (half * units, units), (0, width), "shrink", 0, 0),
            ]
        )
    for pack in packs:
        at = len(sources)
        sources.extend(pack)
        if len(pack) == 1:
            plan.append(whole_entry((at, 0), (at, width), units, width))
        else:
            plan.append(whole_entry((at, 0), (at + 1, 0), units, width))
    vmem = pl.BlockSpec(memory_space=pltpu.VMEM)
    hbm = pl.BlockSpec(memory_space=pl.ANY)
    return pl.pallas_call(
        functools.partial(feed_kernel, plan, units),
        out_shape=jax.ShapeDtypeStruct((rows, width), BF16),
        in_specs=[vmem] * 4 + [hbm] * len(sources),
        out_specs=vmem,
        scratch_shapes=[
            pltpu.VMEM((rows, width), BF16),
            pltpu.VMEM((rows, width), F32),
            pltpu.VMEM((2, width, units), BF16),
            pltpu.VMEM((2, units, width), BF16),
            pltpu.SemaphoreType.DMA((2, 1 + width // units)),
        ],
        compiler_params=params(60),
        cost_estimate=cost(4 * rows * width * units * len(plan), 4 * width * units * len(plan)),
        name="feed",
    )(context, start, gain, project_out, *sources)


def sums_kernel(per_step, table, low, own, high, weights, out, wide, sems):
    step = pl.program_id(0)

    @pl.when(step == 0)
    def _():
        load_wide((low, own, high), wide, sems)

    slots = weights.shape[1]
    for local in range(per_step):
        left, right = gathered_dot(table, weights, wide, step * per_step + local, local, slots)
        back = lax.dot_general(right, left, (((0,), (1,)), ((), ())), preferred_element_type=F32)
        out[0, local : local + 1, :] = jnp.sum(back, axis=0, keepdims=True)
        out[1, local : local + 1, :] = jnp.sum(back * back, axis=0, keepdims=True)


def final_kernel(per_step, table, low, own, high, weights, sums, state, gain, out, wide, sems):
    step = pl.program_id(0)

    @pl.when(step == 0)
    def _():
        load_wide((low, own, high), wide, sems)

    average = sums[0] / D
    scale = lax.rsqrt(sums[1] / D - average * average + EPSILON)
    average = average.T
    scale = scale.T
    slots, rows = weights.shape[1], weights.shape[2]
    for local in range(per_step):
        left, right = gathered_dot(table, weights, wide, step * per_step + local, local, slots)
        back = jnp.dot(left, right, preferred_element_type=F32)
        normed = (back - average[:, local : local + 1]) * scale[:, local : local + 1] * gain[...]
        here = slice(local * rows, (local + 1) * rows)
        out[here, :] = (state[here, :].astype(F32) + normed).astype(BF16)


def decode_specs(low, own, high, weights, per_step):
    _, slots, rows, _ = weights.shape
    wide_rows = low.shape[0] + own.shape[0] + high.shape[0]
    ins = [pl.BlockSpec(memory_space=pl.ANY)] * 3 + [
        pl.BlockSpec((per_step, slots, rows, rows), lambda i, t: (i, 0, 0, 0))
    ]
    scratch = [pltpu.VMEM((wide_rows, own.shape[1]), BF16), pltpu.SemaphoreType.DMA((3,))]
    return ins, scratch


def decode_sums(table, low, own, high, weights):
    blocks, slots, rows, _ = weights.shape
    per_step = 8
    ins, scratch = decode_specs(low, own, high, weights, per_step)
    return pl.pallas_call(
        functools.partial(sums_kernel, per_step),
        out_shape=jax.ShapeDtypeStruct((2, blocks, rows), F32),
        grid_spec=pltpu.PrefetchScalarGridSpec(
            num_scalar_prefetch=1,
            grid=(blocks // per_step,),
            in_specs=ins,
            out_specs=pl.BlockSpec((2, per_step, rows), lambda i, t: (0, i, 0)),
            scratch_shapes=scratch,
        ),
        compiler_params=params(60, ("arbitrary",)),
        name="decode_sums",
    )(table, low, own, high, weights)


def decode_final(table, low, own, high, weights, sums, state, gain):
    blocks, slots, rows, _ = weights.shape
    columns = own.shape[1]
    per_step = 8
    ins, scratch = decode_specs(low, own, high, weights, per_step)
    return pl.pallas_call(
        functools.partial(final_kernel, per_step),
        out_shape=jax.ShapeDtypeStruct(state.shape, BF16),
        grid_spec=pltpu.PrefetchScalarGridSpec(
            num_scalar_prefetch=1,
            grid=(blocks // per_step,),
            in_specs=ins
            + [
                pl.BlockSpec((2, per_step, rows), lambda i, t: (0, i, 0)),
                pl.BlockSpec((per_step * rows, columns), lambda i, t: (i, 0)),
                pl.BlockSpec((1, columns), lambda i, t: (0, 0)),
            ],
            out_specs=pl.BlockSpec((per_step * rows, columns), lambda i, t: (i, 0)),
            scratch_shapes=scratch,
        ),
        compiler_params=params(60, ("arbitrary",)),
        name="decode_final",
    )(table, low, own, high, weights, sums, state, gain)


def spread_weights(expand, shrink, gate):
    core = lax.axis_index("seq") % 2
    units = expand.shape[1] // 2
    mine = lax.dynamic_slice_in_dim(expand, core * units, units, 1)
    rows = lax.dynamic_slice_in_dim(shrink, core * units, units, 0)
    cuts = [rows[:, c * units : (c + 1) * units] for c in range(rows.shape[1] // units)]
    pack = jnp.concatenate([mine] + cuts, axis=0)
    _, pack = lax.optimization_barrier((gate, pack))
    count = lax.axis_size("head")
    if count == 4:
        first, second = flipped(pack, 1), flipped(pack, 2)
        half = pack.shape[0] // 2
        _, upper, lower = lax.optimization_barrier((gate, first[:half], second[half:]))
        packs = [[first], [second], [flipped(upper, 2), flipped(lower, 1)]]
    else:
        packs = [[flipped(pack, j)] for j in range(1, count)]
    bands = lax.axis_size("seq")
    pairs = [(i, i ^ 1) for i in range(bands)]
    return packs + [[lax.ppermute(part, "seq", pairs) for part in entry] for entry in packs]


def on_device(
    grid_state,
    encode_index,
    encode_weights,
    first_gain,
    project_in,
    project_out,
    second_gain,
    expand_weights,
    shrink_weights,
    decode_index,
    decode_weights,
    output_gain,
):
    band_number = lax.axis_index("seq")
    band_count = lax.axis_size("seq")
    head_count = lax.axis_size("head")
    block_rows = encode_weights.shape[2]
    mesh_blocks = encode_weights.shape[0]
    mesh_rows = mesh_blocks * block_rows
    grid_blocks = grid_state.shape[0] // block_rows
    columns = grid_state.shape[1]
    heads_here = columns // HEAD_DIM
    mesh_rim = mesh_blocks // 2

    table = (encode_index - (band_number * grid_blocks - mesh_blocks)).reshape(-1)
    weight_q = project_in[:, 0].reshape(head_count, columns, columns)
    keys = project_in[:, 1].reshape(D, heads_here // 2, 2, HEAD_DIM)
    values = project_in[:, 2].reshape(D, heads_here // 2, 2, HEAD_DIM)
    weight_kv = jnp.stack(
        [keys[:, :, 0], values[:, :, 0], values[:, :, 1], keys[:, :, 1]], axis=2
    ).reshape(head_count, columns, 2 * columns)
    queries, keys_values, low, high, start_share = front(
        band_count,
        head_count,
        table,
        grid_state,
        encode_weights,
        first_gain.reshape(head_count, 1, columns),
        weight_q,
        weight_kv,
    )

    gate = start_share
    held = lax.optimization_barrier((gate, project_out))
    whole_out = lax.all_gather(held[1], "head", axis=0, tiled=True)
    packs = spread_weights(expand_weights, shrink_weights, gate)

    context = attend(
        (band_number * mesh_rows).astype(jnp.int32).reshape(1),
        mesh_rows * band_count,
        queries,
        low,
        keys_values,
        high,
    )
    context_share = lax.all_to_all(context, "head", split_axis=0, concat_axis=1, tiled=True)
    end_share = feed(
        context_share,
        start_share,
        second_gain.reshape(1, D),
        whole_out,
        expand_weights,
        shrink_weights,
        packs,
    )
    mesh_end = lax.all_to_all(end_share, "head", split_axis=1, concat_axis=0, tiled=True)

    low, high = rims(mesh_end, mesh_rim * block_rows)
    table = (decode_index - (band_number * mesh_blocks - mesh_rim)).reshape(-1)
    sums = decode_sums(table, low, mesh_end, high, decode_weights)
    sums = sum(flipped(sums, j) for j in range(1, head_count)) + sums
    return decode_final(
        table, low, mesh_end, high, decode_weights, sums, grid_state, output_gain.reshape(1, columns)
    )


def solution(mesh):
    return jax.shard_map(
        on_device,
        mesh=mesh,
        in_specs=(
            P("seq", "head"),
            P("seq", None),
            P("seq", None, None, None),
            P(),
            P(None, None, "head"),
            P("head", None),
            P(),
            P(None, "head"),
            P("head", None),
            P("seq", None),
            P("seq", None, None, None),
            P("head"),
        ),
        out_specs=P("seq", "head"),
        check_vma=False,
    )
```

```python
import functools

import jax
import jax.numpy as jnp
from jax import lax
from jax.experimental import pallas as pl
from jax.experimental.pallas import tpu as pltpu
from jax.sharding import PartitionSpec as P

D = 1024
HEAD_DIM = 64
WINDOW = 1120
EPSILON = 1e-05
NEGATIVE = -1e30
LOG2_E = 1.4426950408889634
Q_TILE = 256
K_CHUNK = 512
F32 = jnp.float32
BF16 = jnp.bfloat16
MIB = 1024 * 1024
ADVANCE = (2, 3, 4, 6, 7, 8)


def params(mib=48, dims=None):
    return pltpu.CompilerParams(vmem_limit_bytes=mib * MIB, dimension_semantics=dims)


def cost(flops, moved):
    return pl.CostEstimate(flops=int(flops), bytes_accessed=int(moved), transcendentals=0)


def flipped(value, bit):
    count = lax.axis_size("head")
    return lax.ppermute(value, "head", [(i, i ^ bit) for i in range(count)])


def load_wide(parts, wide, sems):
    copies = []
    at = 0
    for number, part in enumerate(parts):
        rows = part.shape[0]
        copies.append(pltpu.make_async_copy(part, wide.at[pl.ds(at, rows)], sems.at[number]))
        at += rows
    for copy in copies:
        copy.start()
    for copy in copies:
        copy.wait()


def gathered_dot(table, weights, wide, block, local, slots):
    rows = weights.shape[2]
    picked = []
    for k in range(slots):
        at = pl.multiple_of(table[block * slots + k] * rows, rows)
        picked.append(wide[pl.ds(at, rows), :])
    left = jnp.concatenate([weights[local, k] for k in range(slots)], axis=1)
    return left, jnp.concatenate(picked, axis=0)


def reach(src, dst, send, recv, **target):
    return pltpu.make_async_remote_copy(
        src_ref=src,
        dst_ref=dst,
        send_sem=send,
        recv_sem=recv,
        device_id=target,
        device_id_type=pl.DeviceIdType.MESH,
    )


def greet(bands, heads, pair=0):
    band = lax.axis_index("seq")
    head = lax.axis_index("head")
    barrier = pltpu.get_barrier_semaphore()
    kind = pl.DeviceIdType.MESH
    for j in range(1, heads):
        pl.semaphore_signal(barrier, inc=1, device_id={"head": head ^ j}, device_id_type=kind)
    if pair:
        pl.semaphore_signal(barrier, inc=1, device_id={"seq": band ^ pair}, device_id_type=kind)

    @pl.when(band > 0)
    def _():
        pl.semaphore_signal(barrier, inc=1, device_id={"seq": band - 1}, device_id_type=kind)

    @pl.when(band < bands - 1)
    def _():
        pl.semaphore_signal(barrier, inc=1, device_id={"seq": band + 1}, device_id_type=kind)

    ends = (band > 0).astype(jnp.int32) + (band < bands - 1).astype(jnp.int32)
    pl.semaphore_wait(barrier, heads - 1 + (1 if pair else 0) + ends)


def front_kernel(bands, heads, rim_rows, *refs):
    table, state, blend, gain, weight_q, weight_kv, project_out = refs[:7]
    out_q, out_kv, out_low, out_high, out_start, out_project = refs[7:13]
    wide, weights, held, q_weights, kv_weights = refs[13:18]
    loads, rim_send, rim_recv, piece_send, piece_recv, kv_send, kv_recv = refs[18:25]
    out_send, out_recv, core_send, core_recv = refs[25:]
    band = lax.axis_index("seq")
    head = lax.axis_index("head")
    blocks, slots, rows, _ = weights.shape
    grid_blocks, _, columns = state.shape
    mesh_rows = blocks * rows
    margin = (wide.shape[0] - grid_blocks) // 2
    chunk = 256
    chunks = mesh_rows // chunk
    has_low = band > 0
    has_high = band < bands - 1
    lower = lax.max(band - 1, 0)
    upper = lax.min(band + 1, bands - 1)

    local = [
        pltpu.make_async_copy(state, wide.at[pl.ds(margin, grid_blocks)], loads.at[0]),
        pltpu.make_async_copy(blend, weights, loads.at[1]),
        pltpu.make_async_copy(weight_q, q_weights, loads.at[2]),
        pltpu.make_async_copy(weight_kv, kv_weights, loads.at[3]),
        pltpu.make_async_copy(project_out, out_project.at[0], loads.at[4]),
    ]
    for copy in local:
        copy.start()
    greet(bands, heads)

    down = reach(
        state.at[pl.ds(0, margin)],
        wide.at[pl.ds(margin + grid_blocks, margin)],
        rim_send.at[0],
        rim_recv.at[1],
        seq=lower,
    )
    up = reach(
        state.at[pl.ds(grid_blocks - margin, margin)],
        wide.at[pl.ds(0, margin)],
        rim_send.at[1],
        rim_recv.at[0],
        seq=upper,
    )
    pl.when(has_low)(down.start)
    pl.when(has_high)(up.start)

    relay = heads == 4
    near = range(1, 3) if relay else range(1, heads)
    cut = project_out.shape[0] // 4

    def part_rows(core, part):
        return pl.ds(pl.multiple_of((core * 2 + part) * cut, cut), cut)

    def project_part(part, owner, partner):
        here = part_rows(band % 2, part)
        source = project_out.at[here] if owner == partner else out_project.at[owner ^ partner, here]
        sems = (out_send.at[owner, part], out_recv.at[owner, part])
        return reach(source, out_project.at[owner, here], *sems, head=head ^ partner)

    def project_core(part, owner, core):
        here = out_project.at[owner, part_rows(core, part)]
        return reach(here, here, core_send.at[owner, part], core_recv.at[owner, part], seq=band ^ 1)

    for part in range(2):
        for j in near:
            project_part(part, j, j).start()

    @pl.when(jnp.logical_not(has_low))
    def _():
        out_low[...] = jnp.zeros(out_low.shape, BF16)

    @pl.when(jnp.logical_not(has_high))
    def _():
        out_high[...] = jnp.zeros(out_high.shape, BF16)

    for copy in local:
        copy.wait()
    pl.when(has_low)(up.wait_recv)
    pl.when(has_high)(down.wait_recv)
    for part in range(2):
        for j in near:
            project_part(part, j, j).wait_recv()
        if relay:
            project_part(part, 3, 2 - part).start()
        for j in near:
            project_core(part, j, band % 2).start()

    def place(step):
        number = jnp.where(band % 2 == 0, step, chunks - 1 - step)
        return number, pl.ds(pl.multiple_of(number * chunk, chunk), chunk)

    def piece(step, owner, partner):
        _, here = place(step)
        source = 0 if owner == partner else owner ^ partner
        return reach(
            held.at[source, here],
            held.at[owner, here],
            piece_send.at[owner, step],
            piece_recv.at[owner, step],
            head=head ^ partner,
        )

    def encode(step):
        number, _ = place(step)
        for part in range(chunk // rows):
            block = number * (chunk // rows) + part
            left = jnp.concatenate([weights[block, k] for k in range(slots)], axis=1)
            right = jnp.concatenate([wide[table[block * slots + k]] for k in range(slots)], axis=0)
            at = pl.multiple_of(number * chunk + part * rows, rows)
            held[0, pl.ds(at, rows), :] = jnp.dot(
                left, right, preferred_element_type=F32
            ).astype(BF16)

    def project(step):
        _, here = place(step)
        values = [held[j, here, :].astype(F32) for j in range(heads)]
        average = sum(jnp.sum(v, axis=1, keepdims=True) for v in values) / D
        centred = [v - average for v in values]
        spread = sum(jnp.sum(c * c, axis=1, keepdims=True) for c in centred) / D
        scale = lax.rsqrt(spread + EPSILON)
        queries, others = 0.0, 0.0
        for j in range(heads):
            owner = head ^ j
            normed = (centred[j] * scale * gain[owner]).astype(BF16)
            queries += jnp.dot(normed, q_weights[owner], preferred_element_type=F32)
            others += jnp.dot(normed, kv_weights[owner], preferred_element_type=F32)
        out_q[here, :] = (queries * (HEAD_DIM ** (-0.5) * LOG2_E)).astype(BF16)
        out_kv[here, :] = others.astype(BF16)

    full, rest = divmod(rim_rows, chunk)
    first = mesh_rows - rim_rows

    def rim_copies(step):
        number, here = place(step)
        start = pl.multiple_of(number * chunk, chunk)
        made = []
        whole = jnp.logical_and(has_low, number < full)
        source = out_kv.at[here]
        target = out_high.at[pl.ds(pl.multiple_of(jnp.minimum(start, (full - 1) * chunk), chunk), chunk)]
        made.append((whole, reach(source, target, kv_send.at[0, step], kv_recv.at[0, number], seq=lower)))
        whole = jnp.logical_and(has_high, number >= chunks - full)
        target = out_low.at[pl.ds(pl.multiple_of(jnp.maximum(start - first, rest), 16), chunk)]
        made.append((whole, reach(source, target, kv_send.at[1, step], kv_recv.at[1, number], seq=upper)))
        if rest:
            part = jnp.logical_and(has_low, number == full)
            source = out_kv.at[pl.ds(full * chunk, rest)]
            target = out_high.at[pl.ds(full * chunk, rest)]
            made.append((part, reach(source, target, kv_send.at[0, step], kv_recv.at[0, number], seq=lower)))
            part = jnp.logical_and(has_high, number == chunks - full - 1)
            source = out_kv.at[pl.ds(first, rest)]
            target = out_low.at[pl.ds(0, rest)]
            made.append((part, reach(source, target, kv_send.at[1, step], kv_recv.at[1, number], seq=upper)))
        return made

    def arrival(way, number, size, at):
        into = (out_high if way == 0 else out_low).at[pl.ds(at, size)]
        spare = kv_send.at[way, 0]
        return reach(into, into, spare, kv_recv.at[way, number], seq=upper if way == 0 else lower)

    def diagonal(step):
        return piece(step, 3, 2) if step % 2 == 0 else piece(step, 3, 1)

    def relayed(step):
        return 1 if step % 2 == 0 else 2

    for step in range(chunks + 2):
        if step < chunks:
            encode(step)
            for j in (range(1, 3) if relay else range(1, heads)):
                piece(step, j, j).start()
        if relay and 1 <= step <= chunks:
            piece(step - 1, relayed(step - 1), relayed(step - 1)).wait_recv()
            diagonal(step - 1).start()
        if step >= 2:
            old = step - 2
            for j in range(1, heads):
                if not (relay and j == relayed(old)):
                    piece(old, j, j).wait_recv()
            project(old)
            for here, copy in rim_copies(old):
                pl.when(here)(copy.start)

    for part in range(2):
        if relay:
            project_part(part, 3, 2 - part).wait()
            project_core(part, 3, band % 2).start()
        for j in near:
            project_part(part, j, j).wait_send()
    for part in range(2):
        for j in range(1, heads):
            project_core(part, j, band % 2).wait_send()
            project_core(part, j, 1 - band % 2).wait_recv()

    share = out_start.shape[1]
    mine = pl.ds(pl.multiple_of(head * share, share), share)
    for j in range(heads):
        out_start[head ^ j] = held[j, mine, :]

    pl.when(has_low)(down.wait_send)
    pl.when(has_high)(up.wait_send)
    for step in range(chunks):
        for j in (range(1, 3) if relay else range(1, heads)):
            piece(step, j, j).wait_send()
        if relay:
            diagonal(step).wait_send()
        for here, copy in rim_copies(step):
            pl.when(here)(copy.wait_send)

    for number in range(full):
        pl.when(has_high)(arrival(0, number, chunk, number * chunk).wait_recv)
        other = chunks - full + number
        pl.when(has_low)(arrival(1, other, chunk, rest + number * chunk).wait_recv)
    if rest:
        pl.when(has_high)(arrival(0, full, rest, full * chunk).wait_recv)
        pl.when(has_low)(arrival(1, chunks - full - 1, rest, 0).wait_recv)


def front(bands, heads, table, state, blend, gain, weight_q, weight_kv, project_out):
    blocks, slots, rows, _ = blend.shape
    grid_rows, columns = state.shape
    grid_blocks = grid_rows // rows
    state = state.reshape(grid_blocks, rows, columns)
    mesh_rows = blocks * rows
    rim_rows = min(mesh_rows, WINDOW)
    chunks = mesh_rows // 256
    vmem = pl.BlockSpec(memory_space=pltpu.VMEM)
    hbm = pl.BlockSpec(memory_space=pl.ANY)
    shape = lambda *sizes: jax.ShapeDtypeStruct(sizes, BF16)
    dma = pltpu.SemaphoreType.DMA
    return pl.pallas_call(
        functools.partial(front_kernel, bands, heads, rim_rows),
        out_shape=[
            shape(mesh_rows, columns),
            shape(mesh_rows, 2 * columns),
            shape(rim_rows, 2 * columns),
            shape(rim_rows, 2 * columns),
            shape(heads, mesh_rows // heads, columns),
            shape(heads, *project_out.shape),
        ],
        in_specs=[pl.BlockSpec(memory_space=pltpu.SMEM), hbm, hbm, vmem, hbm, hbm, hbm],
        out_specs=[vmem] * 6,
        scratch_shapes=[
            pltpu.VMEM((grid_blocks + 2 * blocks, rows, columns), BF16),
            pltpu.VMEM(blend.shape, BF16),
            pltpu.VMEM((heads, mesh_rows, columns), BF16),
            pltpu.VMEM(weight_q.shape, BF16),
            pltpu.VMEM(weight_kv.shape, BF16),
            dma((5,)),
            dma((2,)),
            dma((2,)),
            dma((heads, chunks)),
            dma((heads, chunks)),
            dma((2, chunks)),
            dma((2, chunks)),
            dma((heads, 2)),
            dma((heads, 2)),
            dma((heads, 2)),
            dma((heads, 2)),
        ],
        compiler_params=pltpu.CompilerParams(
            vmem_limit_bytes=60 * MIB, collective_id=0, has_side_effects=True
        ),
        cost_estimate=cost(6 * mesh_rows * D * columns * 20, grid_rows * columns * 4),
        name="front",
    )(table, state, blend, gain, weight_q, weight_kv, project_out)


def middle_kernel(bands, heads, *refs):
    queries, low, own, high, begun, gain, project_out, expand, shrink = refs[:9]
    wide = refs[9]
    keys, values, scores, peaks, masks, sent, context = refs[10:17]
    expands, shrinks, total, normed, finished, loads = refs[17:23]
    context_send, context_recv, gather_send, gather_recv = refs[23:27]
    pair_send, pair_recv, core_send, core_recv = refs[27:31]
    end_send, end_recv, rim_send, rim_recv = refs[31:]
    band = lax.axis_index("seq")
    head = lax.axis_index("head")
    core, half = band % 2, (band // 2) % 2
    lower = lax.max(band - 1, 0)
    upper = lax.min(band + 1, bands - 1)
    has_low = band > 0
    has_high = band < bands - 1
    rows, columns = queries.shape
    rim = low.shape[0]
    count = columns // HEAD_DIM
    width = scores.shape[2]
    chunks = width // K_CHUNK
    tiles = rows // Q_TILE
    share = rows // heads
    per_share = share // Q_TILE
    units = expand.shape[1]
    relay = heads == 4
    near = range(1, 3) if relay else range(1, heads)

    greet(bands, heads, 2)

    parts = [(0, 2), (1, 2), (0, 0), (0, 1), (1, 0), (1, 1)]

    def part_rows(part, its_core, its_half):
        array, kind = parts[part]
        cut = (expand if array == 0 else shrink).shape[0] // 8
        number = 4 + its_half * 2 + its_core if kind == 2 else its_core * 2 + kind
        return (expands, shrinks)[array], pl.ds(pl.multiple_of(number * cut, cut), cut)

    def gathered(part, owner, partner):
        table, here = part_rows(part, core, half)
        if owner == partner:
            source = (expand if parts[part][0] == 0 else shrink).at[here]
        else:
            source = table.at[owner ^ partner, here]
        sems = (gather_send.at[owner, part], gather_recv.at[owner, part])
        return reach(source, table.at[owner, here], *sems, head=head ^ partner)

    def paired(part, owner, its_half):
        table, here = part_rows(part, core, its_half)
        sems = (pair_send.at[owner, part], pair_recv.at[owner, part])
        return reach(table.at[owner, here], table.at[owner, here], *sems, seq=band ^ 2)

    def crossed(part, owner, its_core, other):
        table, here = part_rows(part, its_core, 1 - half if other else half)
        at = part + (len(parts) if other else 0)
        sems = (core_send.at[owner, at], core_recv.at[owner, at])
        return reach(table.at[owner, here], table.at[owner, here], *sems, seq=band ^ 1)

    def spread(part, owner):
        gathered(part, owner, owner).wait_recv()
        crossed(part, owner, core, False).start()
        if part < 2:
            paired(part, owner, half).start()

    def passed(part, owner):
        paired(part, owner, 1 - half).wait_recv()
        crossed(part, owner, core, True).start()

    def advance(part):
        for j in near:
            spread(part, j)
        if relay:
            gathered(part, 3, 2 - part % 2).start()

    def arrived(owner):
        for part in range(len(parts)):
            crossed(part, owner, 1 - core, False).wait_recv()
        for part in range(2):
            crossed(part, owner, 1 - core, True).wait_recv()

    for part in range(len(parts)):
        for j in near:
            gathered(part, j, j).start()
    local = [
        pltpu.make_async_copy(expand, expands.at[0], loads.at[0]),
        pltpu.make_async_copy(shrink, shrinks.at[0], loads.at[1]),
    ]
    for copy in local:
        copy.start()

    lane = lax.broadcasted_iota(jnp.int32, (1, 128), 1)
    for h in range(count):
        lanes = slice(128 * h, 128 * (h + 1))
        is_key = (lane < HEAD_DIM) if h % 2 == 0 else (lane >= HEAD_DIM)
        marker = lane == (HEAD_DIM if h % 2 == 0 else 0)
        at = 0
        for source in (low, own, high):
            size = source.shape[0]
            found = source[:, lanes]
            number = band * rows - rim + at + lax.broadcasted_iota(jnp.int32, (size, 1), 0)
            outside = jnp.logical_or(number < 0, number >= bands * rows)
            mark = jnp.where(jnp.logical_and(outside, marker), NEGATIVE, 0.0).astype(BF16)
            keys[h, at : at + size, :] = jnp.where(is_key, found, mark)
            values[h, at : at + size, :] = jnp.where(is_key, jnp.ones_like(found), found)
            at += size
        end = keys.shape[1] - at
        if end:
            keys[h, at:, :] = jnp.zeros((end, 128), BF16)
            values[h, at:, :] = jnp.zeros((end, 128), BF16)
    q_iota = lax.broadcasted_iota(jnp.int32, (Q_TILE, K_CHUNK), 0)
    k_iota = lax.broadcasted_iota(jnp.int32, (Q_TILE, K_CHUNK), 1)
    for n, c in enumerate((0, chunks - 1)):
        distance = k_iota + c * K_CHUNK - q_iota
        allowed = (distance >= 0) & (distance <= 2 * WINDOW)
        masks[n] = jnp.where(allowed, 0.0, NEGATIVE)

    def where_at(step):
        partner = head ^ (heads - 1 - step // per_share)
        tile = partner * per_share + step % per_share
        return pl.multiple_of(tile * Q_TILE, Q_TILE)

    def context_copy(step):
        mask = heads - 1 - step // per_share
        at = pl.ds(pl.multiple_of((step % per_share) * Q_TILE, Q_TILE), Q_TILE)
        sems = (context_send.at[step], context_recv.at[step])
        return reach(sent.at[step], context.at[head, at], *sems, head=head ^ mask)

    def query_of(start, h):
        pair = queries[pl.ds(start, Q_TILE), 128 * (h // 2) : 128 * (h // 2 + 1)]
        is_key = (lane < HEAD_DIM) if h % 2 == 0 else (lane >= HEAD_DIM)
        marker = lane == (HEAD_DIM if h % 2 == 0 else 0)
        return jnp.where(is_key, pair, jnp.where(marker, 1.0, 0.0).astype(BF16))

    def score_chunk(start, h, query, peak, c):
        key = keys[h, pl.ds(start + c * K_CHUNK, K_CHUNK), :]
        score = lax.dot_general(query, key, (((1,), (1,)), ((), ())), preferred_element_type=F32)
        if c == 0:
            score += masks[0]
        if c == chunks - 1:
            score += masks[1]
        scores[h % 2, :, c * K_CHUNK : (c + 1) * K_CHUNK] = score
        for part in range(K_CHUNK // 128):
            piece = score[:, part * 128 : (part + 1) * 128]
            peak = piece if peak is None else jnp.maximum(peak, piece)
        return peak

    def attend(step, _):
        start = where_at(step)
        outs = []
        peak = None
        query = query_of(start, 0)
        for c in range(chunks):
            peak = score_chunk(start, 0, query, peak, c)
        for h in range(count):
            top = jnp.max(peak, axis=1, keepdims=True)
            found, peak = 0.0, None
            if h + 1 < count:
                query = query_of(start, h + 1)
            for c in range(chunks):
                if h + 1 < count:
                    peak = score_chunk(start, h + 1, query, peak, c)
                power = jnp.exp2(scores[h % 2, :, c * K_CHUNK : (c + 1) * K_CHUNK] - top)
                value = values[h, pl.ds(start + c * K_CHUNK, K_CHUNK), :]
                found += jnp.dot(power.astype(BF16), value, preferred_element_type=F32)
            weight = pltpu.roll(found, HEAD_DIM, 1)
            outs.append(found / weight)
        for g in range(count // 2):
            first, second = outs[2 * g], outs[2 * g + 1]
            both = jnp.where(lane < HEAD_DIM, second, first)
            sent[step, :, 128 * g : 128 * (g + 1)] = pltpu.roll(both, HEAD_DIM, 1).astype(BF16)

        @pl.when(step < (heads - 1) * per_share)
        def _():
            context_copy(step).start()

        for part, when in enumerate(ADVANCE[: len(parts)]):
            if when < tiles:
                pl.when(step == when)(functools.partial(advance, part))
        return 0

    lax.fori_loop(0, tiles, attend, 0)
    for step in range((heads - 1) * per_share, tiles):
        at = (step % per_share) * Q_TILE
        context[head, at : at + Q_TILE, :] = sent[step]
    for part, when in enumerate(ADVANCE[: len(parts)]):
        if when >= tiles:
            advance(part)
    for step in range((heads - 1) * per_share):
        context_copy(step).wait_recv()

    attended = 0.0
    for j in range(heads):
        attended += jnp.dot(context[head ^ j], project_out[j], preferred_element_type=F32)
    start = jnp.concatenate([begun[j] for j in range(heads)], axis=1)
    middle = (start.astype(F32) + attended).astype(BF16).astype(F32)
    total[...] = middle
    average = jnp.mean(middle, axis=1, keepdims=True)
    centred = middle - average
    spread_of = jnp.mean(centred * centred, axis=1, keepdims=True)
    normed[...] = (centred * lax.rsqrt(spread_of + EPSILON) * gain[...]).astype(BF16)
    for copy in local:
        copy.wait()

    def feed(j, here):
        piece = units // 2
        for n in range(2):
            lanes = slice(n * piece, (n + 1) * piece)
            tall = jnp.dot(normed[here, :], expands[j, :, lanes], preferred_element_type=F32)
            hidden = jax.nn.gelu(tall).astype(BF16)
            total[here, :] += jnp.dot(hidden, shrinks[j, lanes, :], preferred_element_type=F32)

    feed(0, slice(0, share))
    if relay:
        for part in range(2):
            for j in near:
                passed(part, j)
        arrived(1)
        feed(1, slice(0, share))
        arrived(2)
        for part in range(2):
            spread(part, 3)
        feed(2, slice(0, share))
        for part in range(2, len(parts)):
            spread(part, 3)
        for part in range(2):
            passed(part, 3)
        arrived(3)
    else:
        for j in range(1, heads):
            for part in range(2):
                passed(part, j)
            arrived(j)
            if j < heads - 1:
                feed(j, slice(0, share))

    blocks, block_rows = wide.shape[0] // 2, wide.shape[1]
    edge = blocks // 2
    part_blocks = finished.shape[2]
    halves = finished.shape[1]

    def end_block(owner, number):
        return owner * halves * part_blocks + number * part_blocks

    def end_copy(mask, number):
        at = pl.ds(edge + end_block(head, number), part_blocks)
        sems = (end_send.at[mask, number], end_recv.at[mask, number])
        return reach(finished.at[head ^ mask, number], wide.at[at], *sems, head=head ^ mask)

    def rim_copies(mask, number):
        block = end_block(head ^ mask, number)
        here = wide.at[pl.ds(edge + block, part_blocks)]
        below = wide.at[pl.ds(edge + blocks + jnp.minimum(block, edge - part_blocks), part_blocks)]
        above_block = jnp.maximum(block - (blocks - edge), 0)
        above = wide.at[pl.ds(above_block, part_blocks)]
        sem = rim_send.at[mask, number]
        down_sem = rim_recv.at[0, jnp.minimum(block, edge - part_blocks) // part_blocks]
        up_sem = rim_recv.at[1, above_block // part_blocks]
        return [
            (jnp.logical_and(has_low, block < edge), reach(here, below, sem, down_sem, seq=lower)),
            (jnp.logical_and(has_high, block >= blocks - edge), reach(here, above, sem, up_sem, seq=upper)),
        ]

    size = share // halves
    for number in range(halves):
        here = slice(number * size, (number + 1) * size)
        feed(heads - 1, here)
        for j in range(heads):
            lanes = slice(j * columns, (j + 1) * columns)
            piece = total[here, lanes].astype(BF16).reshape(part_blocks, block_rows, columns)
            finished[j, number] = piece
        for j in range(heads - 1, 0, -1):
            end_copy(j, number).start()
        wide[pl.ds(edge + end_block(head, number), part_blocks)] = finished[head, number]
        for here, copy in rim_copies(0, number):
            pl.when(here)(copy.start)
    for number in range(halves):
        for j in range(1, heads):
            end_copy(j, number).wait_recv()
            for here, copy in rim_copies(j, number):
                pl.when(here)(copy.start)
    for number in range(edge // part_blocks):
        below = wide.at[pl.ds(edge + blocks + number * part_blocks, part_blocks)]
        above = wide.at[pl.ds(number * part_blocks, part_blocks)]
        spare = rim_send.at[0, 0]
        pl.when(has_high)(reach(below, below, spare, rim_recv.at[0, number], seq=upper).wait_recv)
        pl.when(has_low)(reach(above, above, spare, rim_recv.at[1, number], seq=lower).wait_recv)

    for step in range((heads - 1) * per_share):
        context_copy(step).wait_send()
    for part in range(len(parts)):
        for j in near:
            gathered(part, j, j).wait_send()
        if relay:
            gathered(part, 3, 2 - part % 2).wait_send()
        for j in range(1, heads):
            crossed(part, j, core, False).wait_send()
            if part < 2:
                paired(part, j, half).wait_send()
                crossed(part, j, core, True).wait_send()
    for number in range(halves):
        for j in range(heads):
            if j:
                end_copy(j, number).wait_send()
            for here, copy in rim_copies(j, number):
                pl.when(here)(copy.wait_send)


def middle(bands, heads, block_rows, queries, low, own, high, begun, gain, project_out, expand, shrink):
    rows, columns = queries.shape
    share = rows // heads
    depth, units = expand.shape
    count = columns // HEAD_DIM
    width = -(-(Q_TILE + 2 * WINDOW) // K_CHUNK) * K_CHUNK
    wide_rows = rows - Q_TILE + width
    tiles = rows // Q_TILE
    halves = 2 if share >= 4 * block_rows else 1
    part_blocks = share // halves // block_rows
    blocks = rows // block_rows
    vmem = pl.BlockSpec(memory_space=pltpu.VMEM)
    hbm = pl.BlockSpec(memory_space=pl.ANY)
    dma = pltpu.SemaphoreType.DMA
    return pl.pallas_call(
        functools.partial(middle_kernel, bands, heads),
        out_shape=jax.ShapeDtypeStruct((2 * blocks, block_rows, columns), BF16),
        in_specs=[vmem] * 7 + [hbm] * 2,
        out_specs=vmem,
        scratch_shapes=[
            pltpu.VMEM((count, wide_rows, 128), BF16),
            pltpu.VMEM((count, wide_rows, 128), BF16),
            pltpu.VMEM((2, Q_TILE, width), F32),
            pltpu.VMEM((8, 128), F32),
            pltpu.VMEM((2, Q_TILE, K_CHUNK), F32),
            pltpu.VMEM((tiles, Q_TILE, columns), BF16),
            pltpu.VMEM((heads, share, columns), BF16),
            pltpu.VMEM((heads, depth, units), BF16),
            pltpu.VMEM((heads, units, depth), BF16),
            pltpu.VMEM((share, depth), F32),
            pltpu.VMEM((share, depth), BF16),
            pltpu.VMEM((heads, halves, part_blocks, block_rows, columns), BF16),
            dma((2,)),
            dma((tiles,)),
            dma((tiles,)),
            dma((heads, 6)),
            dma((heads, 6)),
            dma((heads, 2)),
            dma((heads, 2)),
            dma((heads, 8)),
            dma((heads, 8)),
            dma((heads, halves)),
            dma((heads, halves)),
            dma((heads, halves)),
            dma((2, blocks // 2 // part_blocks)),
        ],
        compiler_params=pltpu.CompilerParams(
            vmem_limit_bytes=63 * MIB, collective_id=1, has_side_effects=True
        ),
        cost_estimate=cost(40 * rows * width * columns, rows * columns * 8),
        name="middle",
    )(queries, low, own, high, begun, gain, project_out, expand, shrink)


def sums_kernel(per_step, table, source, weights, out, wide, sems):
    step = pl.program_id(0)

    @pl.when(step == 0)
    def _():
        load_wide((source,), wide, sems)

    slots = weights.shape[1]
    for local in range(per_step):
        left, right = gathered_dot(table, weights, wide, step * per_step + local, local, slots)
        back = lax.dot_general(right, left, (((0,), (1,)), ((), ())), preferred_element_type=F32)
        out[0, local : local + 1, :] = jnp.sum(back, axis=0, keepdims=True)
        out[1, local : local + 1, :] = jnp.sum(back * back, axis=0, keepdims=True)


def final_kernel(per_step, table, source, weights, sums, state, gain, out, wide, sems):
    step = pl.program_id(0)

    @pl.when(step == 0)
    def _():
        load_wide((source,), wide, sems)

    average = sums[0] / D
    scale = lax.rsqrt(sums[1] / D - average * average + EPSILON)
    average = average.T
    scale = scale.T
    slots, rows = weights.shape[1], weights.shape[2]
    for local in range(per_step):
        left, right = gathered_dot(table, weights, wide, step * per_step + local, local, slots)
        back = jnp.dot(left, right, preferred_element_type=F32)
        normed = (back - average[:, local : local + 1]) * scale[:, local : local + 1] * gain[...]
        here = slice(local * rows, (local + 1) * rows)
        out[here, :] = (state[here, :].astype(F32) + normed).astype(BF16)


def decode_specs(source, weights, per_step):
    _, slots, rows, _ = weights.shape
    ins = [pl.BlockSpec(memory_space=pl.ANY)] + [
        pl.BlockSpec((per_step, slots, rows, rows), lambda i, t: (i, 0, 0, 0))
    ]
    scratch = [pltpu.VMEM(source.shape, BF16), pltpu.SemaphoreType.DMA((1,))]
    return ins, scratch


def decode_sums(table, source, weights):
    blocks, slots, rows, _ = weights.shape
    per_step = 8
    ins, scratch = decode_specs(source, weights, per_step)
    return pl.pallas_call(
        functools.partial(sums_kernel, per_step),
        out_shape=jax.ShapeDtypeStruct((2, blocks, rows), F32),
        grid_spec=pltpu.PrefetchScalarGridSpec(
            num_scalar_prefetch=1,
            grid=(blocks // per_step,),
            in_specs=ins,
            out_specs=pl.BlockSpec((2, per_step, rows), lambda i, t: (0, i, 0)),
            scratch_shapes=scratch,
        ),
        compiler_params=params(60, ("arbitrary",)),
        name="decode_sums",
    )(table, source, weights)


def decode_final(table, source, weights, sums, state, gain):
    blocks, slots, rows, _ = weights.shape
    columns = source.shape[1]
    per_step = 8
    ins, scratch = decode_specs(source, weights, per_step)
    return pl.pallas_call(
        functools.partial(final_kernel, per_step),
        out_shape=jax.ShapeDtypeStruct(state.shape, BF16),
        grid_spec=pltpu.PrefetchScalarGridSpec(
            num_scalar_prefetch=1,
            grid=(blocks // per_step,),
            in_specs=ins
            + [
                pl.BlockSpec((2, per_step, rows), lambda i, t: (0, i, 0)),
                pl.BlockSpec((per_step * rows, columns), lambda i, t: (i, 0)),
                pl.BlockSpec((1, columns), lambda i, t: (0, 0)),
            ],
            out_specs=pl.BlockSpec((per_step * rows, columns), lambda i, t: (i, 0)),
            scratch_shapes=scratch,
        ),
        compiler_params=params(60, ("arbitrary",)),
        name="decode_final",
    )(table, source, weights, sums, state, gain)


def on_device(
    grid_state,
    encode_index,
    encode_weights,
    first_gain,
    project_in,
    project_out,
    second_gain,
    expand_weights,
    shrink_weights,
    decode_index,
    decode_weights,
    output_gain,
):
    band_number = lax.axis_index("seq")
    band_count = lax.axis_size("seq")
    head_count = lax.axis_size("head")
    block_rows = encode_weights.shape[2]
    mesh_blocks = encode_weights.shape[0]
    mesh_rows = mesh_blocks * block_rows
    grid_blocks = grid_state.shape[0] // block_rows
    columns = grid_state.shape[1]
    heads_here = columns // HEAD_DIM
    mesh_rim = mesh_blocks // 2

    table = (encode_index - (band_number * grid_blocks - mesh_blocks)).reshape(-1)
    weight_q = project_in[:, 0].reshape(head_count, columns, columns)
    keys = project_in[:, 1].reshape(D, heads_here // 2, 2, HEAD_DIM)
    values = project_in[:, 2].reshape(D, heads_here // 2, 2, HEAD_DIM)
    weight_kv = jnp.stack(
        [keys[:, :, 0], values[:, :, 0], values[:, :, 1], keys[:, :, 1]], axis=2
    ).reshape(head_count, columns, 2 * columns)
    queries, keys_values, low, high, start_share, whole_out = front(
        band_count,
        head_count,
        table,
        grid_state,
        encode_weights,
        first_gain.reshape(head_count, 1, columns),
        weight_q,
        weight_kv,
        project_out,
    )

    wide = middle(
        band_count,
        head_count,
        block_rows,
        queries,
        low,
        keys_values,
        high,
        start_share,
        second_gain.reshape(1, D),
        whole_out,
        expand_weights,
        shrink_weights,
    ).reshape(2 * mesh_rows, columns)
    table = (decode_index - (band_number * mesh_blocks - mesh_rim)).reshape(-1)
    sums = decode_sums(table, wide, decode_weights)
    sums = sum(flipped(sums, j) for j in range(1, head_count)) + sums
    return decode_final(
        table, wide, decode_weights, sums, grid_state, output_gain.reshape(1, columns)
    )


def solution(mesh):
    return jax.shard_map(
        on_device,
        mesh=mesh,
        in_specs=(
            P("seq", "head"),
            P("seq", None),
            P("seq", None, None, None),
            P(),
            P(None, None, "head"),
            P("head", None),
            P(),
            P(None, "head"),
            P("head", None),
            P("seq", None),
            P("seq", None, None, None),
            P("head"),
        ),
        out_specs=P("seq", "head"),
        check_vma=False,
    )
```

```python
import functools

import jax
import jax.numpy as jnp
from jax import lax
from jax.experimental import pallas as pl
from jax.experimental.pallas import tpu as pltpu
from jax.sharding import PartitionSpec as P

D = 1024
HEAD_DIM = 64
WINDOW = 1120
EPSILON = 1e-05
NEGATIVE = -1e30
LOG2_E = 1.4426950408889634
Q_TILE = 256
K_CHUNK = 512
F32 = jnp.float32
BF16 = jnp.bfloat16
MIB = 1024 * 1024
RELAY = 2
BEHIND = 4
SPREAD_STEPS = (2, 3)
FAR_STEPS = (7, 8)
PASS_STEP = 9


def params(mib=48, dims=None):
    return pltpu.CompilerParams(vmem_limit_bytes=mib * MIB, dimension_semantics=dims)


def cost(flops, moved):
    return pl.CostEstimate(flops=int(flops), bytes_accessed=int(moved), transcendentals=0)


def reach(src, dst, send, recv, **target):
    return pltpu.make_async_remote_copy(
        src_ref=src,
        dst_ref=dst,
        send_sem=send,
        recv_sem=recv,
        device_id=target,
        device_id_type=pl.DeviceIdType.MESH,
    )


def greet(bands, heads, pair=0):
    band = lax.axis_index("seq")
    head = lax.axis_index("head")
    barrier = pltpu.get_barrier_semaphore()
    kind = pl.DeviceIdType.MESH
    for j in range(1, heads):
        pl.semaphore_signal(barrier, inc=1, device_id={"head": head ^ j}, device_id_type=kind)
    if pair:
        pl.semaphore_signal(barrier, inc=1, device_id={"seq": band ^ pair}, device_id_type=kind)

    @pl.when(band > 0)
    def _():
        pl.semaphore_signal(barrier, inc=1, device_id={"seq": band - 1}, device_id_type=kind)

    @pl.when(band < bands - 1)
    def _():
        pl.semaphore_signal(barrier, inc=1, device_id={"seq": band + 1}, device_id_type=kind)

    ends = (band > 0).astype(jnp.int32) + (band < bands - 1).astype(jnp.int32)
    pl.semaphore_wait(barrier, heads - 1 + (1 if pair else 0) + ends)


def within(number, ref):
    return jnp.clip(number, 0, ref.shape[0] - 1)


def front_kernel(bands, heads, rim_rows, *refs):
    table, state, blend, gain, project_in, project_out, expand, shrink = refs[:8]
    out_q, out_kv, out_low, out_high, out_start, out_project, out_expand, out_shrink = refs[8:16]
    wide, weights, held, projections = refs[16:20]
    loads, rim_send, rim_recv, piece_send, piece_recv, kv_send, kv_recv = refs[20:27]
    out_send, out_recv, core_send, core_recv = refs[27:31]
    gather_send, gather_recv, pair_send, pair_recv, cross_send, cross_recv = refs[31:]
    band = lax.axis_index("seq")
    head = lax.axis_index("head")
    blocks, slots, rows, _ = weights.shape
    grid_blocks, _, columns = state.shape
    mesh_rows = blocks * rows
    margin = (wide.shape[0] - grid_blocks) // 2
    chunk = 256
    chunks = mesh_rows // chunk
    base = band * grid_blocks - margin
    has_low = band > 0
    has_high = band < bands - 1
    lower = lax.max(band - 1, 0)
    upper = lax.min(band + 1, bands - 1)

    local = [
        pltpu.make_async_copy(state, wide.at[pl.ds(margin, grid_blocks)], loads.at[0]),
        pltpu.make_async_copy(blend, weights, loads.at[1]),
        pltpu.make_async_copy(project_in, projections, loads.at[2]),
        pltpu.make_async_copy(project_out, out_project.at[0], loads.at[3]),
    ]
    for copy in local:
        copy.start()
    greet(bands, heads, 2)

    down = reach(
        state.at[pl.ds(0, margin)],
        wide.at[pl.ds(margin + grid_blocks, margin)],
        rim_send.at[0],
        rim_recv.at[1],
        seq=lower,
    )
    up = reach(
        state.at[pl.ds(grid_blocks - margin, margin)],
        wide.at[pl.ds(0, margin)],
        rim_send.at[1],
        rim_recv.at[0],
        seq=upper,
    )
    pl.when(has_low)(down.start)
    pl.when(has_high)(up.start)

    relay = heads == 4
    near = range(1, 3) if relay else range(1, heads)
    cut = project_out.shape[0] // 4

    def part_rows(core, part):
        return pl.ds(pl.multiple_of((core * 2 + part) * cut, cut), cut)

    def project_part(part, owner, partner):
        here = part_rows(band % 2, part)
        source = project_out.at[here] if owner == partner else out_project.at[owner ^ partner, here]
        sems = (out_send.at[owner, part], out_recv.at[owner, part])
        return reach(source, out_project.at[owner, here], *sems, head=head ^ partner)

    def project_core(part, owner, core):
        here = out_project.at[owner, part_rows(core, part)]
        return reach(here, here, core_send.at[owner, part], core_recv.at[owner, part], seq=band ^ 1)

    half = (band // 2) % 2

    def shared_rows(array, its_core, its_half, base):
        size = (expand, shrink)[array].shape[0] // 8
        return pl.ds(pl.multiple_of((base + its_half * 2 + its_core) * size, size), size)

    def gathered(array, owner, partner):
        table = (out_expand, out_shrink)[array]
        here = shared_rows(array, band % 2, half, 0)
        if owner == partner:
            source = (expand, shrink)[array].at[shared_rows(array, band % 2, half, 4)]
        else:
            source = table.at[owner ^ partner, here]
        sems = (gather_send.at[owner, array], gather_recv.at[owner, array])
        return reach(source, table.at[owner, here], *sems, head=head ^ partner)

    def paired(array, owner, its_half):
        here = (out_expand, out_shrink)[array].at[owner, shared_rows(array, band % 2, its_half, 0)]
        return reach(here, here, pair_send.at[owner, array], pair_recv.at[owner, array], seq=band ^ 2)

    def crossed(array, owner, its_core, other):
        its_half = 1 - half if other else half
        here = (out_expand, out_shrink)[array].at[owner, shared_rows(array, its_core, its_half, 0)]
        at = array + 2 if other else array
        return reach(here, here, cross_send.at[owner, at], cross_recv.at[owner, at], seq=band ^ 1)

    def spread(array, owner):
        gathered(array, owner, owner).wait_recv()
        crossed(array, owner, band % 2, False).start()
        paired(array, owner, half).start()

    def passed(array, owner):
        paired(array, owner, 1 - half).wait_recv()
        crossed(array, owner, band % 2, True).start()

    def advance(array):
        for j in near:
            spread(array, j)
        if relay:
            gathered(array, 3, 2 - array).start()

    for part in range(2):
        for j in near:
            project_part(part, j, j).start()
    for array in range(2):
        for j in near:
            gathered(array, j, j).start()

    @pl.when(jnp.logical_not(has_low))
    def _():
        out_low[...] = jnp.zeros(out_low.shape, BF16)

    @pl.when(jnp.logical_not(has_high))
    def _():
        out_high[...] = jnp.zeros(out_high.shape, BF16)

    for copy in local:
        copy.wait()
    pl.when(has_low)(up.wait_recv)
    pl.when(has_high)(down.wait_recv)
    for part in range(2):
        for j in near:
            project_part(part, j, j).wait_recv()
        if relay:
            project_part(part, 3, 2 - part).start()
        for j in near:
            project_core(part, j, band % 2).start()

    def place(step):
        number = jnp.where(band % 2 == 0, step, chunks - 1 - step)
        return number, pl.ds(pl.multiple_of(number * chunk, chunk), chunk)

    def piece(step, owner, partner):
        _, here = place(step)
        source = 0 if owner == partner else owner ^ partner
        return reach(
            held.at[source, here],
            held.at[owner, here],
            piece_send.at[owner, step],
            piece_recv.at[owner, step],
            head=head ^ partner,
        )

    def encode(step):
        number, _ = place(step)
        for part in range(chunk // rows):
            block = number * (chunk // rows) + part
            left = jnp.concatenate([weights[block, k] for k in range(slots)], axis=1)
            right = jnp.concatenate([wide[within(table[block, k] - base, wide)] for k in range(slots)], axis=0)
            at = pl.multiple_of(number * chunk + part * rows, rows)
            held[0, pl.ds(at, rows), :] = jnp.dot(
                left, right, preferred_element_type=F32
            ).astype(BF16)

    def project(step):
        _, here = place(step)
        values = [held[j, here, :].astype(F32) for j in range(heads)]
        average = sum(jnp.sum(v, axis=1, keepdims=True) for v in values) / D
        centred = [v - average for v in values]
        spread = sum(jnp.sum(c * c, axis=1, keepdims=True) for c in centred) / D
        scale = lax.rsqrt(spread + EPSILON)
        made = [0.0, 0.0, 0.0]
        for j in range(heads):
            owner = head ^ j
            normed = (centred[j] * scale * gain[owner]).astype(BF16)
            lines = pl.ds(pl.multiple_of(owner * columns, columns), columns)
            for t in range(3):
                made[t] += jnp.dot(normed, projections[t, lines, :], preferred_element_type=F32)
        out_q[here, :] = (made[0] * (HEAD_DIM ** (-0.5) * LOG2_E)).astype(BF16)
        out_kv[here, :columns] = made[1].astype(BF16)
        out_kv[here, columns:] = made[2].astype(BF16)

    full, rest = divmod(rim_rows, chunk)
    first = mesh_rows - rim_rows

    def rim_copies(step):
        number, here = place(step)
        start = pl.multiple_of(number * chunk, chunk)
        made = []
        whole = jnp.logical_and(has_low, number < full)
        source = out_kv.at[here]
        target = out_high.at[pl.ds(pl.multiple_of(jnp.minimum(start, (full - 1) * chunk), chunk), chunk)]
        made.append((whole, reach(source, target, kv_send.at[0, step], kv_recv.at[0, number], seq=lower)))
        whole = jnp.logical_and(has_high, number >= chunks - full)
        target = out_low.at[pl.ds(pl.multiple_of(jnp.maximum(start - first, rest), 16), chunk)]
        made.append((whole, reach(source, target, kv_send.at[1, step], kv_recv.at[1, number], seq=upper)))
        if rest:
            part = jnp.logical_and(has_low, number == full)
            source = out_kv.at[pl.ds(full * chunk, rest)]
            target = out_high.at[pl.ds(full * chunk, rest)]
            made.append((part, reach(source, target, kv_send.at[0, step], kv_recv.at[0, number], seq=lower)))
            part = jnp.logical_and(has_high, number == chunks - full - 1)
            source = out_kv.at[pl.ds(first, rest)]
            target = out_low.at[pl.ds(0, rest)]
            made.append((part, reach(source, target, kv_send.at[1, step], kv_recv.at[1, number], seq=upper)))
        return made

    def arrival(way, number, size, at):
        into = (out_high if way == 0 else out_low).at[pl.ds(at, size)]
        spare = kv_send.at[way, 0]
        return reach(into, into, spare, kv_recv.at[way, number], seq=upper if way == 0 else lower)

    def diagonal(step):
        return piece(step, 3, 2) if step % 2 == 0 else piece(step, 3, 1)

    def relayed(step):
        return 1 if step % 2 == 0 else 2

    for step in range(chunks + BEHIND):
        if step < chunks:
            encode(step)
            for j in (range(1, 3) if relay else range(1, heads)):
                piece(step, j, j).start()
        old = step - RELAY
        if relay and 0 <= old < chunks:
            piece(old, relayed(old), relayed(old)).wait_recv()
            diagonal(old).start()
        old = step - BEHIND
        if old >= 0:
            for j in range(1, heads):
                if not (relay and j == relayed(old)):
                    piece(old, j, j).wait_recv()
            project(old)
            for here, copy in rim_copies(old):
                pl.when(here)(copy.start)
        if step in SPREAD_STEPS:
            advance(SPREAD_STEPS.index(step))
        if relay and step in FAR_STEPS:
            spread(FAR_STEPS.index(step), 3)
        if step == PASS_STEP:
            for array in range(2):
                for j in near:
                    passed(array, j)

    for array in range(2):
        if relay:
            passed(array, 3)
    for array in range(2):
        for j in range(1, heads):
            crossed(array, j, 1 - band % 2, False).wait_recv()
            crossed(array, j, 1 - band % 2, True).wait_recv()
            crossed(array, j, band % 2, False).wait_send()
            crossed(array, j, band % 2, True).wait_send()
            paired(array, j, half).wait_send()
            if j in near:
                gathered(array, j, j).wait_send()
            else:
                gathered(array, 3, 2 - array).wait_send()
    for part in range(2):
        if relay:
            project_part(part, 3, 2 - part).wait()
            project_core(part, 3, band % 2).start()
        for j in near:
            project_part(part, j, j).wait_send()
    for part in range(2):
        for j in range(1, heads):
            project_core(part, j, band % 2).wait_send()
            project_core(part, j, 1 - band % 2).wait_recv()

    share = out_start.shape[1]
    mine = pl.ds(pl.multiple_of(head * share, share), share)
    for j in range(heads):
        out_start[head ^ j] = held[j, mine, :]

    pl.when(has_low)(down.wait_send)
    pl.when(has_high)(up.wait_send)
    for step in range(chunks):
        for j in (range(1, 3) if relay else range(1, heads)):
            piece(step, j, j).wait_send()
        if relay:
            diagonal(step).wait_send()
        for here, copy in rim_copies(step):
            pl.when(here)(copy.wait_send)

    for number in range(full):
        pl.when(has_high)(arrival(0, number, chunk, number * chunk).wait_recv)
        other = chunks - full + number
        pl.when(has_low)(arrival(1, other, chunk, rest + number * chunk).wait_recv)
    if rest:
        pl.when(has_high)(arrival(0, full, rest, full * chunk).wait_recv)
        pl.when(has_low)(arrival(1, chunks - full - 1, rest, 0).wait_recv)


def front(bands, heads, table, state, blend, gain, *others):
    project_in, project_out, expand, shrink = others
    blocks, slots, rows, _ = blend.shape
    grid_rows, columns = state.shape
    grid_blocks = grid_rows // rows
    state = state.reshape(grid_blocks, rows, columns)
    mesh_rows = blocks * rows
    rim_rows = min(mesh_rows, WINDOW)
    chunks = mesh_rows // 256
    vmem = pl.BlockSpec(memory_space=pltpu.VMEM)
    hbm = pl.BlockSpec(memory_space=pl.ANY)
    shape = lambda *sizes: jax.ShapeDtypeStruct(sizes, BF16)
    dma = pltpu.SemaphoreType.DMA
    return pl.pallas_call(
        functools.partial(front_kernel, bands, heads, rim_rows),
        out_shape=[
            shape(mesh_rows, columns),
            shape(mesh_rows, 2 * columns),
            shape(rim_rows, 2 * columns),
            shape(rim_rows, 2 * columns),
            shape(heads, mesh_rows // heads, columns),
            shape(heads, *project_out.shape),
            shape(heads, expand.shape[0] // 2, expand.shape[1]),
            shape(heads, shrink.shape[0] // 2, shrink.shape[1]),
        ],
        in_specs=[pl.BlockSpec(memory_space=pltpu.SMEM), hbm, hbm, vmem] + [hbm] * 4,
        out_specs=[vmem] * 6 + [hbm] * 2,
        scratch_shapes=[
            pltpu.VMEM((grid_blocks + 2 * blocks, rows, columns), BF16),
            pltpu.VMEM(blend.shape, BF16),
            pltpu.VMEM((heads, mesh_rows, columns), BF16),
            pltpu.VMEM(project_in.shape, BF16),
            dma((4,)),
            dma((2,)),
            dma((2,)),
            dma((heads, chunks)),
            dma((heads, chunks)),
            dma((2, chunks)),
            dma((2, chunks)),
            *[dma((heads, 2))] * 8,
            *[dma((heads, 4))] * 2,
        ],
        compiler_params=pltpu.CompilerParams(
            vmem_limit_bytes=60 * MIB, collective_id=0, has_side_effects=True
        ),
        cost_estimate=cost(6 * mesh_rows * D * columns * 20, grid_rows * columns * 4),
        name="front",
    )(table, state, blend, gain, *others)


def middle_kernel(bands, heads, *refs):
    queries, low, own, high, begun, gain, project_out, expand, shrink, half_e, half_s = refs[:11]
    wide = refs[11]
    keys, values, scores, masks, sent, context = refs[12:18]
    expands, shrinks, total, normed, finished, loads = refs[18:24]
    context_send, context_recv, gather_send, gather_recv, core_send, core_recv = refs[24:30]
    end_send, end_recv, rim_send, rim_recv = refs[30:]
    band = lax.axis_index("seq")
    head = lax.axis_index("head")
    core = band % 2
    lower = lax.max(band - 1, 0)
    upper = lax.min(band + 1, bands - 1)
    has_low = band > 0
    has_high = band < bands - 1
    rows, columns = queries.shape
    rim = low.shape[0]
    count = columns // HEAD_DIM
    width = scores.shape[2]
    chunks = width // K_CHUNK
    tiles = rows // Q_TILE
    share = rows // heads
    per_share = share // Q_TILE
    units = expand.shape[1]
    relay = heads == 4
    near = range(1, 3) if relay else range(1, heads)

    greet(bands, heads)

    parts = [(0, 0), (0, 1), (1, 0), (1, 1)]

    def part_rows(part, its_core):
        array, kind = parts[part]
        cut = (expand if array == 0 else shrink).shape[0] // 8
        return (expands, shrinks)[array], pl.ds(pl.multiple_of((its_core * 2 + kind) * cut, cut), cut)

    def gathered(part, owner, partner):
        table, here = part_rows(part, core)
        if owner == partner:
            source = (expand if parts[part][0] == 0 else shrink).at[here]
        else:
            source = table.at[owner ^ partner, here]
        sems = (gather_send.at[owner, part], gather_recv.at[owner, part])
        return reach(source, table.at[owner, here], *sems, head=head ^ partner)

    def crossed(part, owner, its_core):
        table, here = part_rows(part, its_core)
        sems = (core_send.at[owner, part], core_recv.at[owner, part])
        return reach(table.at[owner, here], table.at[owner, here], *sems, seq=band ^ 1)

    def spread(part, owner):
        gathered(part, owner, owner).wait_recv()
        crossed(part, owner, core).start()

    def advance(part):
        for j in near:
            spread(part, j)
        if relay:
            gathered(part, 3, 2 - part % 2).start()

    def begin(part):
        for j in near:
            gathered(part, j, j).start()

    def arrived(owner):
        for part in range(len(parts)):
            crossed(part, owner, 1 - core).wait_recv()

    begin(0)
    begin(1)
    local = [
        pltpu.make_async_copy(expand, expands.at[0], loads.at[0]),
        pltpu.make_async_copy(shrink, shrinks.at[0], loads.at[1]),
    ]
    for j in range(1, heads):
        for array, (half, table) in enumerate(((half_e, expands), (half_s, shrinks))):
            size = half.shape[1]
            local.append(
                pltpu.make_async_copy(half.at[j], table.at[j, pl.ds(size, size)], loads.at[2 * j + array])
            )
    for copy in local:
        copy.start()

    lane = lax.broadcasted_iota(jnp.int32, (1, 128), 1)
    for h in range(count):
        lanes = slice(128 * (h // 2), 128 * (h // 2 + 1))
        value_lanes = slice(columns + 128 * (h // 2), columns + 128 * (h // 2 + 1))
        is_mine = (lane < HEAD_DIM) if h % 2 == 0 else (lane >= HEAD_DIM)
        marker = lane == (HEAD_DIM if h % 2 == 0 else 0)
        at = 0
        for source in (low, own, high):
            size = source.shape[0]
            number = band * rows - rim + at + lax.broadcasted_iota(jnp.int32, (size, 1), 0)
            outside = jnp.logical_or(number < 0, number >= bands * rows)
            mark = jnp.where(jnp.logical_and(outside, marker), NEGATIVE, 0.0).astype(BF16)
            keys[h, at : at + size, :] = jnp.where(is_mine, source[:, lanes], mark)
            found = source[:, value_lanes]
            values[h, at : at + size, :] = jnp.where(is_mine, found, jnp.ones_like(found))
            at += size
        end = keys.shape[1] - at
        if end:
            keys[h, at:, :] = jnp.zeros((end, 128), BF16)
            values[h, at:, :] = jnp.zeros((end, 128), BF16)
    q_iota = lax.broadcasted_iota(jnp.int32, (Q_TILE, K_CHUNK), 0)
    k_iota = lax.broadcasted_iota(jnp.int32, (Q_TILE, K_CHUNK), 1)
    for n, c in enumerate((0, chunks - 1)):
        distance = k_iota + c * K_CHUNK - q_iota
        allowed = (distance >= 0) & (distance <= 2 * WINDOW)
        masks[n] = jnp.where(allowed, 0.0, NEGATIVE)

    def where_at(step):
        partner = head ^ (heads - 1 - step // per_share)
        tile = partner * per_share + step % per_share
        return pl.multiple_of(tile * Q_TILE, Q_TILE)

    def context_copy(step):
        mask = heads - 1 - step // per_share
        at = pl.ds(pl.multiple_of((step % per_share) * Q_TILE, Q_TILE), Q_TILE)
        sems = (context_send.at[step], context_recv.at[step])
        return reach(sent.at[step], context.at[head, at], *sems, head=head ^ mask)

    def query_of(start, h):
        pair = queries[pl.ds(start, Q_TILE), 128 * (h // 2) : 128 * (h // 2 + 1)]
        is_key = (lane < HEAD_DIM) if h % 2 == 0 else (lane >= HEAD_DIM)
        marker = lane == (HEAD_DIM if h % 2 == 0 else 0)
        return jnp.where(is_key, pair, jnp.where(marker, 1.0, 0.0).astype(BF16))

    def score_chunk(start, h, query, peak, c):
        key = keys[h, pl.ds(start + c * K_CHUNK, K_CHUNK), :]
        score = lax.dot_general(query, key, (((1,), (1,)), ((), ())), preferred_element_type=F32)
        if c == 0:
            score += masks[0]
        if c == chunks - 1:
            score += masks[1]
        scores[h % 2, :, c * K_CHUNK : (c + 1) * K_CHUNK] = score
        for part in range(K_CHUNK // 128):
            piece = score[:, part * 128 : (part + 1) * 128]
            peak = piece if peak is None else jnp.maximum(peak, piece)
        return peak

    def attend(step, _):
        start = where_at(step)
        outs = []
        peak = None
        query = query_of(start, 0)
        for c in range(chunks):
            peak = score_chunk(start, 0, query, peak, c)
        for h in range(count):
            top = jnp.max(peak, axis=1, keepdims=True)
            found, peak = 0.0, None
            if h + 1 < count:
                query = query_of(start, h + 1)
            for c in range(chunks):
                if h + 1 < count:
                    peak = score_chunk(start, h + 1, query, peak, c)
                power = jnp.exp2(scores[h % 2, :, c * K_CHUNK : (c + 1) * K_CHUNK] - top)
                value = values[h, pl.ds(start + c * K_CHUNK, K_CHUNK), :]
                found += jnp.dot(power.astype(BF16), value, preferred_element_type=F32)
            weight = pltpu.roll(found, HEAD_DIM, 1)
            outs.append(found / weight)
        for g in range(count // 2):
            first, second = outs[2 * g], outs[2 * g + 1]
            both = jnp.where(lane < HEAD_DIM, first, second)
            sent[step, :, 128 * g : 128 * (g + 1)] = both.astype(BF16)

        @pl.when(step < (heads - 1) * per_share)
        def _():
            context_copy(step).start()

        @pl.when(step == (heads - 1) * per_share)
        def _():
            begin(2)
            begin(3)
            advance(0)
            advance(1)

        return 0

    lax.fori_loop(0, tiles, attend, 0)
    for step in range((heads - 1) * per_share, tiles):
        at = (step % per_share) * Q_TILE
        context[head, at : at + Q_TILE, :] = sent[step]
    for step in range((heads - 1) * per_share):
        context_copy(step).wait_recv()

    attended = 0.0
    for j in range(heads):
        attended += jnp.dot(context[head ^ j], project_out[j], preferred_element_type=F32)
    start = jnp.concatenate([begun[j] for j in range(heads)], axis=1)
    middle = (start.astype(F32) + attended).astype(BF16).astype(F32)
    total[...] = middle
    average = jnp.mean(middle, axis=1, keepdims=True)
    centred = middle - average
    spread_of = jnp.mean(centred * centred, axis=1, keepdims=True)
    normed[...] = (centred * lax.rsqrt(spread_of + EPSILON) * gain[...]).astype(BF16)
    for copy in local:
        copy.wait()

    def feed(j, here):
        piece = units // 2
        for n in range(2):
            lanes = slice(n * piece, (n + 1) * piece)
            tall = jnp.dot(normed[here, :], expands[j, :, lanes], preferred_element_type=F32)
            hidden = jax.nn.gelu(tall).astype(BF16)
            total[here, :] += jnp.dot(hidden, shrinks[j, lanes, :], preferred_element_type=F32)

    advance(2)
    feed(0, slice(0, share))
    advance(3)
    for j in range(1, heads):
        if relay and j == 3:
            for part in range(len(parts)):
                spread(part, 3)
        arrived(j)
        if j < heads - 1:
            feed(j, slice(0, share))

    blocks, block_rows = wide.shape[0] // 2, wide.shape[1]
    edge = blocks // 2
    part_blocks = finished.shape[2]
    halves = finished.shape[1]

    def end_block(owner, number):
        return owner * halves * part_blocks + number * part_blocks

    def end_copy(mask, number):
        at = pl.ds(edge + end_block(head, number), part_blocks)
        sems = (end_send.at[mask, number], end_recv.at[mask, number])
        return reach(finished.at[head ^ mask, number], wide.at[at], *sems, head=head ^ mask)

    def rim_copies(mask, number):
        block = end_block(head ^ mask, number)
        here = wide.at[pl.ds(edge + block, part_blocks)]
        below = wide.at[pl.ds(edge + blocks + jnp.minimum(block, edge - part_blocks), part_blocks)]
        above_block = jnp.maximum(block - (blocks - edge), 0)
        above = wide.at[pl.ds(above_block, part_blocks)]
        sem = rim_send.at[mask, number]
        down_sem = rim_recv.at[0, jnp.minimum(block, edge - part_blocks) // part_blocks]
        up_sem = rim_recv.at[1, above_block // part_blocks]
        return [
            (jnp.logical_and(has_low, block < edge), reach(here, below, sem, down_sem, seq=lower)),
            (jnp.logical_and(has_high, block >= blocks - edge), reach(here, above, sem, up_sem, seq=upper)),
        ]

    size = share // halves
    for number in range(halves):
        here = slice(number * size, (number + 1) * size)
        feed(heads - 1, here)
        for j in range(heads):
            lanes = slice(j * columns, (j + 1) * columns)
            piece = total[here, lanes].astype(BF16).reshape(part_blocks, block_rows, columns)
            finished[j, number] = piece
        for j in range(heads - 1, 0, -1):
            end_copy(j, number).start()
        wide[pl.ds(edge + end_block(head, number), part_blocks)] = finished[head, number]
        for here, copy in rim_copies(0, number):
            pl.when(here)(copy.start)
    for number in range(halves):
        for j in range(1, heads):
            end_copy(j, number).wait_recv()
            for here, copy in rim_copies(j, number):
                pl.when(here)(copy.start)
    for number in range(edge // part_blocks):
        below = wide.at[pl.ds(edge + blocks + number * part_blocks, part_blocks)]
        above = wide.at[pl.ds(number * part_blocks, part_blocks)]
        spare = rim_send.at[0, 0]
        pl.when(has_high)(reach(below, below, spare, rim_recv.at[0, number], seq=upper).wait_recv)
        pl.when(has_low)(reach(above, above, spare, rim_recv.at[1, number], seq=lower).wait_recv)

    for step in range((heads - 1) * per_share):
        context_copy(step).wait_send()
    for part in range(len(parts)):
        for j in near:
            gathered(part, j, j).wait_send()
        if relay:
            gathered(part, 3, 2 - part % 2).wait_send()
        for j in range(1, heads):
            crossed(part, j, core).wait_send()
    for number in range(halves):
        for j in range(heads):
            if j:
                end_copy(j, number).wait_send()
            for here, copy in rim_copies(j, number):
                pl.when(here)(copy.wait_send)


def middle(bands, heads, block_rows, queries, *others):
    expand = others[6]
    rows, columns = queries.shape
    share = rows // heads
    depth, units = expand.shape
    count = columns // HEAD_DIM
    width = -(-(Q_TILE + 2 * WINDOW) // K_CHUNK) * K_CHUNK
    wide_rows = rows - Q_TILE + width
    tiles = rows // Q_TILE
    halves = 2 if share >= 4 * block_rows else 1
    part_blocks = share // halves // block_rows
    blocks = rows // block_rows
    vmem = pl.BlockSpec(memory_space=pltpu.VMEM)
    hbm = pl.BlockSpec(memory_space=pl.ANY)
    dma = pltpu.SemaphoreType.DMA
    return pl.pallas_call(
        functools.partial(middle_kernel, bands, heads),
        out_shape=jax.ShapeDtypeStruct((2 * blocks, block_rows, columns), BF16),
        in_specs=[vmem] * 7 + [hbm] * 4,
        out_specs=vmem,
        scratch_shapes=[
            pltpu.VMEM((count, wide_rows, 128), BF16),
            pltpu.VMEM((count, wide_rows, 128), BF16),
            pltpu.VMEM((2, Q_TILE, width), F32),
            pltpu.VMEM((2, Q_TILE, K_CHUNK), F32),
            pltpu.VMEM((tiles, Q_TILE, columns), BF16),
            pltpu.VMEM((heads, share, columns), BF16),
            pltpu.VMEM((heads, depth, units), BF16),
            pltpu.VMEM((heads, units, depth), BF16),
            pltpu.VMEM((share, depth), F32),
            pltpu.VMEM((share, depth), BF16),
            pltpu.VMEM((heads, halves, part_blocks, block_rows, columns), BF16),
            dma((2 * heads,)),
            dma((tiles,)),
            dma((tiles,)),
            *[dma((heads, 4))] * 4,
            dma((heads, halves)),
            dma((heads, halves)),
            dma((heads, halves)),
            dma((2, blocks // 2 // part_blocks)),
        ],
        compiler_params=pltpu.CompilerParams(
            vmem_limit_bytes=63 * MIB, collective_id=1, has_side_effects=True
        ),
        cost_estimate=cost(40 * rows * width * columns, rows * columns * 8),
        name="middle",
    )(queries, *others)


def decode_kernel(heads, *refs):
    table, source, weights_in, state_in, gain, out = refs[:6]
    wide, weights, state, backs, sums, packed, theirs, loads, stores, send, recv = refs[6:]
    head = lax.axis_index("head")
    barrier = pltpu.get_barrier_semaphore()
    groups, group, rows, columns = backs.shape
    slots = weights.shape[2]
    per_half = groups // 2
    half_blocks = per_half * group
    edge = wide.shape[0] // 4
    base = lax.axis_index("seq") * 2 * edge - edge

    loads_of = [pltpu.make_async_copy(source, wide, loads.at[0])]
    for g in range(groups):
        loads_of.append(pltpu.make_async_copy(weights_in.at[g], weights.at[g], loads.at[1 + g]))
    state_load = pltpu.make_async_copy(state_in, state, loads.at[1 + groups])
    for copy in loads_of:
        copy.start()
    state_load.start()
    for j in range(1, heads):
        pl.semaphore_signal(
            barrier, inc=1, device_id={"head": head ^ j}, device_id_type=pl.DeviceIdType.MESH
        )
    pl.semaphore_wait(barrier, heads - 1)

    def exchange(part, j):
        sems = (send.at[part, j], recv.at[part, j])
        return reach(packed.at[part], theirs.at[part, j], *sems, head=head ^ j)

    lane = lax.broadcasted_iota(jnp.int32, (rows, 128), 1)
    loads_of[0].wait()
    sums[...] = jnp.zeros(sums.shape, F32)
    for part in range(2):

        def gather(inner, _):
            g = part * per_half + inner
            pltpu.make_async_copy(weights_in.at[g], weights.at[g], loads.at[1 + g]).wait()
            found = sums[part]
            for local in range(group):
                block = g * group + local
                left = jnp.concatenate([weights[g, local, k] for k in range(slots)], axis=1)
                right = jnp.concatenate([wide[within(table[block, k] - base, wide)] for k in range(slots)], axis=0)
                back = jnp.dot(left, right, preferred_element_type=F32)
                backs[g, local] = back
                once = jnp.sum(back, axis=1, keepdims=True)
                twice = jnp.sum(back * back, axis=1, keepdims=True)
                at = inner * group + local
                found = jnp.where(lane == at, once, found)
                found = jnp.where(lane == at + half_blocks, twice, found)
            sums[part] = found
            return 0

        lax.fori_loop(0, per_half, gather, 0)
        found = sums[part]
        lower = pltpu.roll(found[rows // 2 :], 64, 1)
        packed[part] = jnp.where(lane[: rows // 2] < 64, found[: rows // 2], lower)
        for j in range(1, heads):
            exchange(part, j).start()

    state_load.wait()
    for part in range(2):
        for j in range(1, heads):
            exchange(part, j).wait_recv()
        whole = packed[part]
        for j in range(1, heads):
            whole = whole + theirs[part, j]
        whole = jnp.concatenate([whole, pltpu.roll(whole, 64, 1)], axis=0) / D
        squares = pltpu.roll(whole, 128 - half_blocks, 1)
        sums[part] = jnp.where(lane < half_blocks, whole, 0.0)
        scale = lax.rsqrt(squares - whole * whole + EPSILON)
        scale = pltpu.roll(jnp.where(lane < half_blocks, scale, 0.0), half_blocks, 1)
        sums[part] = jnp.where(lane < half_blocks, whole, scale)

        def finish(inner, _):
            g = part * per_half + inner
            here = pltpu.roll(sums[part], lax.rem(128 - inner * group, 128), 1)
            for local in range(group):
                average = here[:, local : local + 1]
                scale = here[:, half_blocks + local : half_blocks + local + 1]
                normed = (backs[g, local] - average) * scale * gain[...]
                state[g, local] = (state[g, local].astype(F32) + normed).astype(BF16)
            pltpu.make_async_copy(state.at[g], out.at[g], stores.at[g]).start()
            return 0

        lax.fori_loop(0, per_half, finish, 0)
    for g in range(groups):
        pltpu.make_async_copy(state.at[g], out.at[g], stores.at[g]).wait()
    for part in range(2):
        for j in range(1, heads):
            exchange(part, j).wait_send()


def decode(heads, table, source, weights, state, gain):
    blocks, slots, rows, _ = weights.shape
    columns = state.shape[1]
    group = 8
    groups = blocks // group
    weights = weights.reshape(groups, group, slots, rows, rows)
    shape = state.shape
    state = state.reshape(groups, group, rows, columns)
    hbm = pl.BlockSpec(memory_space=pl.ANY)
    vmem = pl.BlockSpec(memory_space=pltpu.VMEM)
    dma = pltpu.SemaphoreType.DMA
    return pl.pallas_call(
        functools.partial(decode_kernel, heads),
        out_shape=jax.ShapeDtypeStruct(state.shape, BF16),
        in_specs=[pl.BlockSpec(memory_space=pltpu.SMEM), hbm, hbm, hbm, vmem],
        out_specs=hbm,
        scratch_shapes=[
            pltpu.VMEM(source.shape, BF16),
            pltpu.VMEM(weights.shape, BF16),
            pltpu.VMEM(state.shape, BF16),
            pltpu.VMEM(state.shape, F32),
            pltpu.VMEM((2, rows, 128), F32),
            pltpu.VMEM((2, rows // 2, 128), F32),
            pltpu.VMEM((2, heads, rows // 2, 128), F32),
            dma((2 + groups,)),
            dma((groups,)),
            dma((2, heads)),
            dma((2, heads)),
        ],
        compiler_params=pltpu.CompilerParams(
            vmem_limit_bytes=63 * MIB, collective_id=2, has_side_effects=True
        ),
        cost_estimate=cost(8 * blocks * rows * rows * columns, 6 * blocks * rows * columns),
        name="decode",
    )(table, source, weights, state, gain).reshape(shape)


def on_device(
    grid_state,
    encode_index,
    encode_weights,
    first_gain,
    project_in,
    project_out,
    second_gain,
    expand_weights,
    shrink_weights,
    decode_index,
    decode_weights,
    output_gain,
):
    band_number = lax.axis_index("seq")
    band_count = lax.axis_size("seq")
    head_count = lax.axis_size("head")
    block_rows = encode_weights.shape[2]
    mesh_blocks = encode_weights.shape[0]
    mesh_rows = mesh_blocks * block_rows
    grid_blocks = grid_state.shape[0] // block_rows
    columns = grid_state.shape[1]
    heads_here = columns // HEAD_DIM
    mesh_rim = mesh_blocks // 2

    queries, keys_values, low, high, start_share, whole_out, expands, shrinks = front(
        band_count,
        head_count,
        encode_index,
        grid_state,
        encode_weights,
        first_gain.reshape(head_count, 1, columns),
        project_in.transpose(1, 0, 2),
        project_out,
        expand_weights,
        shrink_weights,
    )

    wide = middle(
        band_count,
        head_count,
        block_rows,
        queries,
        low,
        keys_values,
        high,
        start_share,
        second_gain.reshape(1, D),
        whole_out,
        expand_weights,
        shrink_weights,
        expands,
        shrinks,
    )
    return decode(
        head_count, decode_index, wide, decode_weights, grid_state, output_gain.reshape(1, columns)
    )


def solution(mesh):
    return jax.shard_map(
        on_device,
        mesh=mesh,
        in_specs=(
            P("seq", "head"),
            P("seq", None),
            P("seq", None, None, None),
            P(),
            P(None, None, "head"),
            P("head", None),
            P(),
            P(None, "head"),
            P("head", None),
            P("seq", None),
            P("seq", None, None, None),
            P("head"),
        ),
        out_specs=P("seq", "head"),
        check_vma=False,
    )
```

```python
import functools

import jax
import jax.numpy as jnp
from jax import lax
from jax.experimental import pallas as pl
from jax.experimental.pallas import tpu as pltpu
from jax.sharding import PartitionSpec as P

D = 1024
HEAD_DIM = 64
WINDOW = 1120
EPSILON = 1e-05
NEGATIVE = -1e30
LOG2_E = 1.4426950408889634
Q_TILE = 256
K_CHUNK = 512
F32 = jnp.float32
BF16 = jnp.bfloat16
MIB = 1024 * 1024
RELAY = 2
BEHIND = 3
SPREAD_STEPS = (1, 1)
FAR_STEPS = (4, 5)
PASS_STEP = 8


def params(mib=48, dims=None):
    return pltpu.CompilerParams(vmem_limit_bytes=mib * MIB, dimension_semantics=dims)


def cost(flops, moved):
    return pl.CostEstimate(flops=int(flops), bytes_accessed=int(moved), transcendentals=0)


def reach(src, dst, send, recv, **target):
    return pltpu.make_async_remote_copy(
        src_ref=src,
        dst_ref=dst,
        send_sem=send,
        recv_sem=recv,
        device_id=target,
        device_id_type=pl.DeviceIdType.MESH,
    )


def greet(bands, heads, pair=0):
    band = lax.axis_index("seq")
    head = lax.axis_index("head")
    barrier = pltpu.get_barrier_semaphore()
    kind = pl.DeviceIdType.MESH
    for j in range(1, heads):
        pl.semaphore_signal(barrier, inc=1, device_id={"head": head ^ j}, device_id_type=kind)
    if pair:
        pl.semaphore_signal(barrier, inc=1, device_id={"seq": band ^ pair}, device_id_type=kind)

    @pl.when(band > 0)
    def _():
        pl.semaphore_signal(barrier, inc=1, device_id={"seq": band - 1}, device_id_type=kind)

    @pl.when(band < bands - 1)
    def _():
        pl.semaphore_signal(barrier, inc=1, device_id={"seq": band + 1}, device_id_type=kind)

    ends = (band > 0).astype(jnp.int32) + (band < bands - 1).astype(jnp.int32)
    pl.semaphore_wait(barrier, heads - 1 + (1 if pair else 0) + ends)


def within(number, ref):
    return jnp.clip(number, 0, ref.shape[0] - 1)


def front_kernel(bands, heads, rim_rows, *refs):
    table, state, blend, gain, project_in, project_out, expand, shrink = refs[:8]
    out_q, out_kv, out_low, out_high, out_start, out_project, out_expand, out_shrink = refs[8:16]
    wide, weights, held, projections = refs[16:20]
    loads, rim_send, rim_recv, piece_send, piece_recv, kv_send, kv_recv = refs[20:27]
    out_send, out_recv, core_send, core_recv = refs[27:31]
    gather_send, gather_recv, pair_send, pair_recv, cross_send, cross_recv = refs[31:]
    band = lax.axis_index("seq")
    head = lax.axis_index("head")
    blocks, slots, rows, _ = weights.shape
    grid_blocks, _, columns = state.shape
    mesh_rows = blocks * rows
    margin = (wide.shape[0] - grid_blocks) // 2
    chunk = 256
    chunks = mesh_rows // chunk
    base = band * grid_blocks - margin
    has_low = band > 0
    has_high = band < bands - 1
    lower = lax.max(band - 1, 0)
    upper = lax.min(band + 1, bands - 1)

    local = [
        pltpu.make_async_copy(state, wide.at[pl.ds(margin, grid_blocks)], loads.at[0]),
        pltpu.make_async_copy(blend, weights, loads.at[1]),
        pltpu.make_async_copy(project_in, projections, loads.at[2]),
        pltpu.make_async_copy(project_out, out_project.at[0], loads.at[3]),
    ]
    for copy in local:
        copy.start()
    greet(bands, heads, 2)

    down = reach(
        state.at[pl.ds(0, margin)],
        wide.at[pl.ds(margin + grid_blocks, margin)],
        rim_send.at[0],
        rim_recv.at[1],
        seq=lower,
    )
    up = reach(
        state.at[pl.ds(grid_blocks - margin, margin)],
        wide.at[pl.ds(0, margin)],
        rim_send.at[1],
        rim_recv.at[0],
        seq=upper,
    )
    pl.when(has_low)(down.start)
    pl.when(has_high)(up.start)

    relay = heads == 4
    near = range(1, 3) if relay else range(1, heads)
    cut = project_out.shape[0] // 4

    def part_rows(core, part):
        return pl.ds(pl.multiple_of((core * 2 + part) * cut, cut), cut)

    def project_part(part, owner, partner):
        here = part_rows(band % 2, part)
        source = project_out.at[here] if owner == partner else out_project.at[owner ^ partner, here]
        sems = (out_send.at[owner, part], out_recv.at[owner, part])
        return reach(source, out_project.at[owner, here], *sems, head=head ^ partner)

    def project_core(part, owner, core):
        here = out_project.at[owner, part_rows(core, part)]
        return reach(here, here, core_send.at[owner, part], core_recv.at[owner, part], seq=band ^ 1)

    half = (band // 2) % 2

    def shared_rows(array, its_core, its_half, base):
        size = (expand, shrink)[array].shape[0] // 8
        return pl.ds(pl.multiple_of((base + its_half * 2 + its_core) * size, size), size)

    def gathered(array, owner, partner):
        table = (out_expand, out_shrink)[array]
        here = shared_rows(array, band % 2, half, 0)
        if owner == partner:
            source = (expand, shrink)[array].at[shared_rows(array, band % 2, half, 4)]
        else:
            source = table.at[owner ^ partner, here]
        sems = (gather_send.at[owner, array], gather_recv.at[owner, array])
        return reach(source, table.at[owner, here], *sems, head=head ^ partner)

    def paired(array, owner, its_half):
        here = (out_expand, out_shrink)[array].at[owner, shared_rows(array, band % 2, its_half, 0)]
        return reach(here, here, pair_send.at[owner, array], pair_recv.at[owner, array], seq=band ^ 2)

    def crossed(array, owner, its_core, other):
        its_half = 1 - half if other else half
        here = (out_expand, out_shrink)[array].at[owner, shared_rows(array, its_core, its_half, 0)]
        at = array + 2 if other else array
        return reach(here, here, cross_send.at[owner, at], cross_recv.at[owner, at], seq=band ^ 1)

    def spread(array, owner):
        gathered(array, owner, owner).wait_recv()
        crossed(array, owner, band % 2, False).start()
        paired(array, owner, half).start()

    def passed(array, owner):
        paired(array, owner, 1 - half).wait_recv()
        crossed(array, owner, band % 2, True).start()

    def advance(array):
        for j in near:
            spread(array, j)
        if relay:
            gathered(array, 3, 2 - array).start()

    for part in range(2):
        for j in near:
            project_part(part, j, j).start()
    for array in range(2):
        for j in near:
            gathered(array, j, j).start()

    @pl.when(jnp.logical_not(has_low))
    def _():
        out_low[...] = jnp.zeros(out_low.shape, BF16)

    @pl.when(jnp.logical_not(has_high))
    def _():
        out_high[...] = jnp.zeros(out_high.shape, BF16)

    for copy in local:
        copy.wait()
    pl.when(has_low)(up.wait_recv)
    pl.when(has_high)(down.wait_recv)
    for part in range(2):
        for j in near:
            project_part(part, j, j).wait_recv()
        if relay:
            project_part(part, 3, 2 - part).start()
        for j in near:
            project_core(part, j, band % 2).start()

    def place(step):
        number = jnp.where(band % 2 == 0, step, chunks - 1 - step)
        return number, pl.ds(pl.multiple_of(number * chunk, chunk), chunk)

    def piece(step, owner, partner):
        _, here = place(step)
        source = 0 if owner == partner else owner ^ partner
        return reach(
            held.at[source, here],
            held.at[owner, here],
            piece_send.at[owner, step],
            piece_recv.at[owner, step],
            head=head ^ partner,
        )

    def encode(step):
        number, _ = place(step)
        for part in range(chunk // rows):
            block = number * (chunk // rows) + part
            left = jnp.concatenate([weights[block, k] for k in range(slots)], axis=1)
            right = jnp.concatenate([wide[within(table[block, k] - base, wide)] for k in range(slots)], axis=0)
            at = pl.multiple_of(number * chunk + part * rows, rows)
            held[0, pl.ds(at, rows), :] = jnp.dot(
                left, right, preferred_element_type=F32
            ).astype(BF16)

    def project(step):
        _, here = place(step)
        values = [held[j, here, :].astype(F32) for j in range(heads)]
        average = sum(jnp.sum(v, axis=1, keepdims=True) for v in values) / D
        centred = [v - average for v in values]
        spread = sum(jnp.sum(c * c, axis=1, keepdims=True) for c in centred) / D
        scale = lax.rsqrt(spread + EPSILON)
        made = [0.0, 0.0, 0.0]
        for j in range(heads):
            owner = head ^ j
            normed = (centred[j] * scale * gain[owner]).astype(BF16)
            lines = pl.ds(pl.multiple_of(owner * columns, columns), columns)
            for t in range(3):
                made[t] += jnp.dot(normed, projections[t, lines, :], preferred_element_type=F32)
        out_q[here, :] = (made[0] * (HEAD_DIM ** (-0.5) * LOG2_E)).astype(BF16)
        out_kv[here, :columns] = made[1].astype(BF16)
        out_kv[here, columns:] = made[2].astype(BF16)

    full, rest = divmod(rim_rows, chunk)
    first = mesh_rows - rim_rows

    def rim_copies(step):
        number, here = place(step)
        start = pl.multiple_of(number * chunk, chunk)
        made = []
        whole = jnp.logical_and(has_low, number < full)
        source = out_kv.at[here]
        target = out_high.at[pl.ds(pl.multiple_of(jnp.minimum(start, (full - 1) * chunk), chunk), chunk)]
        made.append((whole, reach(source, target, kv_send.at[0, step], kv_recv.at[0, number], seq=lower)))
        whole = jnp.logical_and(has_high, number >= chunks - full)
        target = out_low.at[pl.ds(pl.multiple_of(jnp.maximum(start - first, rest), 16), chunk)]
        made.append((whole, reach(source, target, kv_send.at[1, step], kv_recv.at[1, number], seq=upper)))
        if rest:
            part = jnp.logical_and(has_low, number == full)
            source = out_kv.at[pl.ds(full * chunk, rest)]
            target = out_high.at[pl.ds(full * chunk, rest)]
            made.append((part, reach(source, target, kv_send.at[0, step], kv_recv.at[0, number], seq=lower)))
            part = jnp.logical_and(has_high, number == chunks - full - 1)
            source = out_kv.at[pl.ds(first, rest)]
            target = out_low.at[pl.ds(0, rest)]
            made.append((part, reach(source, target, kv_send.at[1, step], kv_recv.at[1, number], seq=upper)))
        return made

    def arrival(way, number, size, at):
        into = (out_high if way == 0 else out_low).at[pl.ds(at, size)]
        spare = kv_send.at[way, 0]
        return reach(into, into, spare, kv_recv.at[way, number], seq=upper if way == 0 else lower)

    def diagonal(step):
        return piece(step, 3, 2) if step % 2 == 0 else piece(step, 3, 1)

    def relayed(step):
        return 1 if step % 2 == 0 else 2

    for step in range(chunks + BEHIND):
        if step < chunks:
            encode(step)
            for j in (range(1, 3) if relay else range(1, heads)):
                piece(step, j, j).start()
        old = step - RELAY
        if relay and 0 <= old < chunks:
            piece(old, relayed(old), relayed(old)).wait_recv()
            diagonal(old).start()
        old = step - BEHIND
        if old >= 0:
            for j in range(1, heads):
                if not (relay and j == relayed(old)):
                    piece(old, j, j).wait_recv()
            project(old)
            for here, copy in rim_copies(old):
                pl.when(here)(copy.start)
        if step == 1:
            advance(0)
            advance(1)
        if relay and step in FAR_STEPS:
            spread(FAR_STEPS.index(step), 3)
        if step == PASS_STEP:
            for array in range(2):
                for j in near:
                    passed(array, j)

    for array in range(2):
        if relay:
            passed(array, 3)
    for array in range(2):
        for j in range(1, heads):
            crossed(array, j, 1 - band % 2, False).wait_recv()
            crossed(array, j, 1 - band % 2, True).wait_recv()
            crossed(array, j, band % 2, False).wait_send()
            crossed(array, j, band % 2, True).wait_send()
            paired(array, j, half).wait_send()
            if j in near:
                gathered(array, j, j).wait_send()
            else:
                gathered(array, 3, 2 - array).wait_send()
    for part in range(2):
        if relay:
            project_part(part, 3, 2 - part).wait()
            project_core(part, 3, band % 2).start()
        for j in near:
            project_part(part, j, j).wait_send()
    for part in range(2):
        for j in range(1, heads):
            project_core(part, j, band % 2).wait_send()
            project_core(part, j, 1 - band % 2).wait_recv()

    share = out_start.shape[1]
    mine = pl.ds(pl.multiple_of(head * share, share), share)
    for j in range(heads):
        out_start[head ^ j] = held[j, mine, :]

    pl.when(has_low)(down.wait_send)
    pl.when(has_high)(up.wait_send)
    for step in range(chunks):
        for j in (range(1, 3) if relay else range(1, heads)):
            piece(step, j, j).wait_send()
        if relay:
            diagonal(step).wait_send()
        for here, copy in rim_copies(step):
            pl.when(here)(copy.wait_send)

    for number in range(full):
        pl.when(has_high)(arrival(0, number, chunk, number * chunk).wait_recv)
        other = chunks - full + number
        pl.when(has_low)(arrival(1, other, chunk, rest + number * chunk).wait_recv)
    if rest:
        pl.when(has_high)(arrival(0, full, rest, full * chunk).wait_recv)
        pl.when(has_low)(arrival(1, chunks - full - 1, rest, 0).wait_recv)


def front(bands, heads, table, state, blend, gain, *others):
    project_in, project_out, expand, shrink = others
    blocks, slots, rows, _ = blend.shape
    grid_rows, columns = state.shape
    grid_blocks = grid_rows // rows
    state = state.reshape(grid_blocks, rows, columns)
    mesh_rows = blocks * rows
    rim_rows = min(mesh_rows, WINDOW)
    chunks = mesh_rows // 256
    vmem = pl.BlockSpec(memory_space=pltpu.VMEM)
    hbm = pl.BlockSpec(memory_space=pl.ANY)
    shape = lambda *sizes: jax.ShapeDtypeStruct(sizes, BF16)
    dma = pltpu.SemaphoreType.DMA
    return pl.pallas_call(
        functools.partial(front_kernel, bands, heads, rim_rows),
        out_shape=[
            shape(mesh_rows, columns),
            shape(mesh_rows, 2 * columns),
            shape(rim_rows, 2 * columns),
            shape(rim_rows, 2 * columns),
            shape(heads, mesh_rows // heads, columns),
            shape(heads, *project_out.shape),
            shape(heads, expand.shape[0] // 2, expand.shape[1]),
            shape(heads, shrink.shape[0] // 2, shrink.shape[1]),
        ],
        in_specs=[pl.BlockSpec(memory_space=pltpu.SMEM), hbm, hbm, vmem] + [hbm] * 4,
        out_specs=[vmem] * 6 + [hbm] * 2,
        scratch_shapes=[
            pltpu.VMEM((grid_blocks + 2 * blocks, rows, columns), BF16),
            pltpu.VMEM(blend.shape, BF16),
            pltpu.VMEM((heads, mesh_rows, columns), BF16),
            pltpu.VMEM(project_in.shape, BF16),
            dma((4,)),
            dma((2,)),
            dma((2,)),
            dma((heads, chunks)),
            dma((heads, chunks)),
            dma((2, chunks)),
            dma((2, chunks)),
            *[dma((heads, 2))] * 8,
            *[dma((heads, 4))] * 2,
        ],
        compiler_params=pltpu.CompilerParams(
            vmem_limit_bytes=60 * MIB, collective_id=0, has_side_effects=True
        ),
        cost_estimate=cost(6 * mesh_rows * D * columns * 20, grid_rows * columns * 4),
        name="front",
    )(table, state, blend, gain, *others)


def middle_kernel(bands, heads, *refs):
    queries, low, own, high, begun, gain, project_out, expand, shrink, half_e, half_s = refs[:11]
    wide = refs[11]
    keys, values, scores, masks, sent, context = refs[12:18]
    expands, shrinks, total, normed, finished, loads = refs[18:24]
    context_send, context_recv, gather_send, gather_recv, core_send, core_recv = refs[24:30]
    pair_send, pair_recv, end_send, end_recv, rim_send, rim_recv = refs[30:]
    band = lax.axis_index("seq")
    head = lax.axis_index("head")
    core, half = band % 2, (band // 2) % 2
    lower = lax.max(band - 1, 0)
    upper = lax.min(band + 1, bands - 1)
    has_low = band > 0
    has_high = band < bands - 1
    rows, columns = queries.shape
    rim = low.shape[0]
    count = columns // HEAD_DIM
    width = scores.shape[2]
    chunks = width // K_CHUNK
    tiles = rows // Q_TILE
    share = rows // heads
    per_share = share // Q_TILE
    units = expand.shape[1]
    relay = heads == 4
    near = range(1, 3) if relay else range(1, heads)

    greet(bands, heads, 2)

    parts = [(1, 2), (0, 0), (0, 1)]

    def part_rows(part, its_core, its_half, split=None):
        array, kind = parts[part]
        size = (expand if array == 0 else shrink).shape[0] // 8
        number = (its_half if kind == 2 else kind) + its_core * 2
        at = number * size
        if split is not None:
            size //= 2
            at += split * size
        return (expands, shrinks)[array], pl.ds(pl.multiple_of(at, size), size)

    def gathered(part, owner):
        table, here = part_rows(part, core, half)
        source = (expand if parts[part][0] == 0 else shrink).at[here]
        sems = (gather_send.at[owner, part], gather_recv.at[owner, part])
        return reach(source, table.at[owner, here], *sems, head=head ^ owner)

    def far(part, split):
        table, here = part_rows(part, core, half, split)
        sems = (gather_send.at[3 * split, part], gather_recv.at[3 * split, part])
        return reach(table.at[1 + split, here], table.at[3, here], *sems, head=head ^ (2 - split))

    def paired(part, owner, its_half):
        table, here = part_rows(part, core, its_half)
        here = table.at[owner, here]
        return reach(here, here, pair_send.at[owner], pair_recv.at[owner], seq=band ^ 2)

    def crossed(part, owner, its_core, other=False):
        table, here = part_rows(part, its_core, 1 - half if other else half)
        here, at = table.at[owner, here], len(parts) if other else part
        return reach(here, here, core_send.at[owner, at], core_recv.at[owner, at], seq=band ^ 1)

    def spread(part, owner):
        if relay and owner == 3:
            far(part, 0).wait_recv()
            far(part, 1).wait_recv()
        else:
            gathered(part, owner).wait_recv()
        if part == 0:
            paired(part, owner, half).start()
        crossed(part, owner, core).start()

    def passed(owner):
        paired(0, owner, 1 - half).wait_recv()
        crossed(0, owner, core, True).start()

    def advance(part):
        for j in near:
            spread(part, j)
        if relay:
            far(part, 0).start()
            far(part, 1).start()

    def begin(part):
        for j in near:
            gathered(part, j).start()

    def arrived(owner):
        for part in range(len(parts)):
            crossed(part, owner, 1 - core).wait_recv()
        crossed(0, owner, 1 - core, True).wait_recv()

    begin(0)
    begin(1)
    local = [
        pltpu.make_async_copy(expand, expands.at[0], loads.at[0]),
        pltpu.make_async_copy(shrink, shrinks.at[0], loads.at[1]),
    ]
    for j in range(1, heads):
        for array, (given, table) in enumerate(((half_e, expands), (half_s, shrinks))):
            size = given.shape[1]
            local.append(
                pltpu.make_async_copy(given.at[j], table.at[j, pl.ds(size, size)], loads.at[2 * j + array])
            )
    for copy in local:
        copy.start()

    lane = lax.broadcasted_iota(jnp.int32, (1, 128), 1)
    for h in range(count):
        lanes = slice(128 * (h // 2), 128 * (h // 2 + 1))
        value_lanes = slice(columns + 128 * (h // 2), columns + 128 * (h // 2 + 1))
        is_mine = (lane < HEAD_DIM) if h % 2 == 0 else (lane >= HEAD_DIM)
        marker = lane == (HEAD_DIM if h % 2 == 0 else 0)
        at = 0
        for source in (low, own, high):
            size = source.shape[0]
            number = band * rows - rim + at + lax.broadcasted_iota(jnp.int32, (size, 1), 0)
            outside = jnp.logical_or(number < 0, number >= bands * rows)
            mark = jnp.where(jnp.logical_and(outside, marker), NEGATIVE, 0.0).astype(BF16)
            keys[h, at : at + size, :] = jnp.where(is_mine, source[:, lanes], mark)
            found = source[:, value_lanes]
            values[h, at : at + size, :] = jnp.where(is_mine, found, jnp.ones_like(found))
            at += size
        end = keys.shape[1] - at
        if end:
            keys[h, at:, :] = jnp.zeros((end, 128), BF16)
            values[h, at:, :] = jnp.zeros((end, 128), BF16)
    q_iota = lax.broadcasted_iota(jnp.int32, (Q_TILE, K_CHUNK), 0)
    k_iota = lax.broadcasted_iota(jnp.int32, (Q_TILE, K_CHUNK), 1)
    for n, c in enumerate((0, chunks - 1)):
        distance = k_iota + c * K_CHUNK - q_iota
        allowed = (distance >= 0) & (distance <= 2 * WINDOW)
        masks[n] = jnp.where(allowed, 0.0, NEGATIVE)

    def where_at(step):
        partner = head ^ (heads - 1 - step // per_share)
        tile = partner * per_share + step % per_share
        return pl.multiple_of(tile * Q_TILE, Q_TILE)

    def context_copy(step):
        mask = heads - 1 - step // per_share
        at = pl.ds(pl.multiple_of((step % per_share) * Q_TILE, Q_TILE), Q_TILE)
        sems = (context_send.at[step], context_recv.at[step])
        return reach(sent.at[step], context.at[head, at], *sems, head=head ^ mask)

    def query_of(start, h):
        pair = queries[pl.ds(start, Q_TILE), 128 * (h // 2) : 128 * (h // 2 + 1)]
        is_key = (lane < HEAD_DIM) if h % 2 == 0 else (lane >= HEAD_DIM)
        marker = lane == (HEAD_DIM if h % 2 == 0 else 0)
        return jnp.where(is_key, pair, jnp.where(marker, 1.0, 0.0).astype(BF16))

    def score_chunk(start, h, query, peak, c):
        key = keys[h, pl.ds(start + c * K_CHUNK, K_CHUNK), :]
        score = lax.dot_general(query, key, (((1,), (1,)), ((), ())), preferred_element_type=F32)
        if c == 0:
            score += masks[0]
        if c == chunks - 1:
            score += masks[1]
        scores[h % 2, :, c * K_CHUNK : (c + 1) * K_CHUNK] = score
        for part in range(K_CHUNK // 128):
            piece = score[:, part * 128 : (part + 1) * 128]
            peak = piece if peak is None else jnp.maximum(peak, piece)
        return peak

    def attend(step, _):
        start = where_at(step)
        outs = []
        peak = None
        query = query_of(start, 0)
        for c in range(chunks):
            peak = score_chunk(start, 0, query, peak, c)
        for h in range(count):
            top = jnp.max(peak, axis=1, keepdims=True)
            found, peak = 0.0, None
            if h + 1 < count:
                query = query_of(start, h + 1)
            for c in range(chunks):
                if h + 1 < count:
                    peak = score_chunk(start, h + 1, query, peak, c)
                power = jnp.exp2(scores[h % 2, :, c * K_CHUNK : (c + 1) * K_CHUNK] - top)
                value = values[h, pl.ds(start + c * K_CHUNK, K_CHUNK), :]
                found += jnp.dot(power.astype(BF16), value, preferred_element_type=F32)
            weight = pltpu.roll(found, HEAD_DIM, 1)
            outs.append(found / weight)
        for g in range(count // 2):
            first, second = outs[2 * g], outs[2 * g + 1]
            both = jnp.where(lane < HEAD_DIM, first, second)
            sent[step, :, 128 * g : 128 * (g + 1)] = both.astype(BF16)

        @pl.when(step < (heads - 1) * per_share)
        def _():
            context_copy(step).start()

        @pl.when(step == (heads - 1) * per_share)
        def _():
            begin(2)
            advance(0)
            advance(1)

        return 0

    lax.fori_loop(0, tiles, attend, 0)
    for step in range((heads - 1) * per_share, tiles):
        at = (step % per_share) * Q_TILE
        context[head, at : at + Q_TILE, :] = sent[step]
    for step in range((heads - 1) * per_share):
        context_copy(step).wait_recv()

    attended = 0.0
    for j in range(heads):
        attended += jnp.dot(context[head ^ j], project_out[j], preferred_element_type=F32)
    start = jnp.concatenate([begun[j] for j in range(heads)], axis=1)
    middle = (start.astype(F32) + attended).astype(BF16).astype(F32)
    total[...] = middle
    average = jnp.mean(middle, axis=1, keepdims=True)
    centred = middle - average
    spread_of = jnp.mean(centred * centred, axis=1, keepdims=True)
    normed[...] = (centred * lax.rsqrt(spread_of + EPSILON) * gain[...]).astype(BF16)
    for copy in local:
        copy.wait()

    def feed(j, here):
        piece = units // 2
        for n in range(2):
            lanes = slice(n * piece, (n + 1) * piece)
            tall = jnp.dot(normed[here, :], expands[j, :, lanes], preferred_element_type=F32)
            hidden = jax.nn.gelu(tall).astype(BF16)
            total[here, :] += jnp.dot(hidden, shrinks[j, lanes, :], preferred_element_type=F32)

    advance(2)
    feed(0, slice(0, share))
    for j in near:
        passed(j)
    if relay:
        spread(0, 3)
    for j in range(1, heads):
        if relay and j == 2:
            spread(1, 3)
        if relay and j == 3:
            spread(2, 3)
            passed(3)
        arrived(j)
        if j < heads - 1:
            feed(j, slice(0, share))

    blocks, block_rows = wide.shape[0] // 2, wide.shape[1]
    edge = blocks // 2
    part_blocks = finished.shape[2]
    halves = finished.shape[1]

    def end_block(owner, number):
        return owner * halves * part_blocks + number * part_blocks

    def end_copy(mask, number):
        at = pl.ds(edge + end_block(head, number), part_blocks)
        sems = (end_send.at[mask, number], end_recv.at[mask, number])
        return reach(finished.at[head ^ mask, number], wide.at[at], *sems, head=head ^ mask)

    def rim_copies(mask, number):
        block = end_block(head ^ mask, number)
        here = wide.at[pl.ds(edge + block, part_blocks)]
        below = wide.at[pl.ds(edge + blocks + jnp.minimum(block, edge - part_blocks), part_blocks)]
        above_block = jnp.maximum(block - (blocks - edge), 0)
        above = wide.at[pl.ds(above_block, part_blocks)]
        sem = rim_send.at[mask, number]
        down_sem = rim_recv.at[0, jnp.minimum(block, edge - part_blocks) // part_blocks]
        up_sem = rim_recv.at[1, above_block // part_blocks]
        return [
            (jnp.logical_and(has_low, block < edge), reach(here, below, sem, down_sem, seq=lower)),
            (jnp.logical_and(has_high, block >= blocks - edge), reach(here, above, sem, up_sem, seq=upper)),
        ]

    size = share // halves
    for number in range(halves):
        here = slice(number * size, (number + 1) * size)
        feed(heads - 1, here)
        for j in range(heads):
            lanes = slice(j * columns, (j + 1) * columns)
            piece = total[here, lanes].astype(BF16).reshape(part_blocks, block_rows, columns)
            finished[j, number] = piece
        for j in range(heads - 1, 0, -1):
            end_copy(j, number).start()
        wide[pl.ds(edge + end_block(head, number), part_blocks)] = finished[head, number]
        for here, copy in rim_copies(0, number):
            pl.when(here)(copy.start)
    for number in range(halves):
        for j in range(1, heads):
            end_copy(j, number).wait_recv()
            for here, copy in rim_copies(j, number):
                pl.when(here)(copy.start)
    for number in range(edge // part_blocks):
        below = wide.at[pl.ds(edge + blocks + number * part_blocks, part_blocks)]
        above = wide.at[pl.ds(number * part_blocks, part_blocks)]
        spare = rim_send.at[0, 0]
        pl.when(has_high)(reach(below, below, spare, rim_recv.at[0, number], seq=upper).wait_recv)
        pl.when(has_low)(reach(above, above, spare, rim_recv.at[1, number], seq=lower).wait_recv)

    for step in range((heads - 1) * per_share):
        context_copy(step).wait_send()
    for part in range(len(parts)):
        for j in near:
            gathered(part, j).wait_send()
        if relay:
            far(part, 0).wait_send()
            far(part, 1).wait_send()
        for j in range(1, heads):
            crossed(part, j, core).wait_send()
    for j in range(1, heads):
        paired(0, j, half).wait_send()
        crossed(0, j, core, True).wait_send()
    for number in range(halves):
        for j in range(heads):
            if j:
                end_copy(j, number).wait_send()
            for here, copy in rim_copies(j, number):
                pl.when(here)(copy.wait_send)


def middle(bands, heads, block_rows, queries, *others):
    expand = others[6]
    rows, columns = queries.shape
    share = rows // heads
    depth, units = expand.shape
    count = columns // HEAD_DIM
    width = -(-(Q_TILE + 2 * WINDOW) // K_CHUNK) * K_CHUNK
    wide_rows = rows - Q_TILE + width
    tiles = rows // Q_TILE
    halves = 2 if share >= 4 * block_rows else 1
    part_blocks = share // halves // block_rows
    blocks = rows // block_rows
    vmem = pl.BlockSpec(memory_space=pltpu.VMEM)
    hbm = pl.BlockSpec(memory_space=pl.ANY)
    dma = pltpu.SemaphoreType.DMA
    return pl.pallas_call(
        functools.partial(middle_kernel, bands, heads),
        out_shape=jax.ShapeDtypeStruct((2 * blocks, block_rows, columns), BF16),
        in_specs=[vmem] * 7 + [hbm] * 4,
        out_specs=vmem,
        scratch_shapes=[
            pltpu.VMEM((count, wide_rows, 128), BF16),
            pltpu.VMEM((count, wide_rows, 128), BF16),
            pltpu.VMEM((2, Q_TILE, width), F32),
            pltpu.VMEM((2, Q_TILE, K_CHUNK), F32),
            pltpu.VMEM((tiles, Q_TILE, columns), BF16),
            pltpu.VMEM((heads, share, columns), BF16),
            pltpu.VMEM((heads, depth, units), BF16),
            pltpu.VMEM((heads, units, depth), BF16),
            pltpu.VMEM((share, depth), F32),
            pltpu.VMEM((share, depth), BF16),
            pltpu.VMEM((heads, halves, part_blocks, block_rows, columns), BF16),
            dma((2 * heads,)),
            dma((tiles,)),
            dma((tiles,)),
            *[dma((heads, 4))] * 4,
            *[dma((heads,))] * 2,
            dma((heads, halves)),
            dma((heads, halves)),
            dma((heads, halves)),
            dma((2, blocks // 2 // part_blocks)),
        ],
        compiler_params=pltpu.CompilerParams(
            vmem_limit_bytes=63 * MIB, collective_id=1, has_side_effects=True
        ),
        cost_estimate=cost(40 * rows * width * columns, rows * columns * 8),
        name="middle",
    )(queries, *others)


def decode_kernel(heads, *refs):
    table, source, weights_in, state_in, gain, out = refs[:6]
    wide, weights, state, backs, sums, packed, theirs, loads, stores, send, recv = refs[6:]
    head = lax.axis_index("head")
    barrier = pltpu.get_barrier_semaphore()
    groups, group, rows, columns = backs.shape
    slots = weights.shape[2]
    per_half = groups // 2
    half_blocks = per_half * group
    edge = wide.shape[0] // 4
    base = lax.axis_index("seq") * 2 * edge - edge

    loads_of = [pltpu.make_async_copy(source, wide, loads.at[0])]
    for g in range(groups):
        loads_of.append(pltpu.make_async_copy(weights_in.at[g], weights.at[g], loads.at[1 + g]))
    state_load = pltpu.make_async_copy(state_in, state, loads.at[1 + groups])
    for copy in loads_of:
        copy.start()
    state_load.start()
    for j in range(1, heads):
        pl.semaphore_signal(
            barrier, inc=1, device_id={"head": head ^ j}, device_id_type=pl.DeviceIdType.MESH
        )
    pl.semaphore_wait(barrier, heads - 1)

    def exchange(part, j):
        sems = (send.at[part, j], recv.at[part, j])
        return reach(packed.at[part], theirs.at[part, j], *sems, head=head ^ j)

    lane = lax.broadcasted_iota(jnp.int32, (rows, 128), 1)
    loads_of[0].wait()
    sums[...] = jnp.zeros(sums.shape, F32)
    for part in range(2):

        def gather(inner, _):
            g = part * per_half + inner
            pltpu.make_async_copy(weights_in.at[g], weights.at[g], loads.at[1 + g]).wait()
            found = sums[part]
            for local in range(group):
                block = g * group + local
                left = jnp.concatenate([weights[g, local, k] for k in range(slots)], axis=1)
                right = jnp.concatenate([wide[within(table[block, k] - base, wide)] for k in range(slots)], axis=0)
                back = jnp.dot(left, right, preferred_element_type=F32)
                backs[g, local] = back
                once = jnp.sum(back, axis=1, keepdims=True)
                twice = jnp.sum(back * back, axis=1, keepdims=True)
                at = inner * group + local
                found = jnp.where(lane == at, once, found)
                found = jnp.where(lane == at + half_blocks, twice, found)
            sums[part] = found
            return 0

        lax.fori_loop(0, per_half, gather, 0)
        found = sums[part]
        lower = pltpu.roll(found[rows // 2 :], 64, 1)
        packed[part] = jnp.where(lane[: rows // 2] < 64, found[: rows // 2], lower)
        for j in range(1, heads):
            exchange(part, j).start()

    state_load.wait()
    for part in range(2):
        for j in range(1, heads):
            exchange(part, j).wait_recv()
        whole = packed[part]
        for j in range(1, heads):
            whole = whole + theirs[part, j]
        whole = jnp.concatenate([whole, pltpu.roll(whole, 64, 1)], axis=0) / D
        squares = pltpu.roll(whole, 128 - half_blocks, 1)
        sums[part] = jnp.where(lane < half_blocks, whole, 0.0)
        scale = lax.rsqrt(squares - whole * whole + EPSILON)
        scale = pltpu.roll(jnp.where(lane < half_blocks, scale, 0.0), half_blocks, 1)
        sums[part] = jnp.where(lane < half_blocks, whole, scale)

        def finish(inner, _):
            g = part * per_half + inner
            here = pltpu.roll(sums[part], lax.rem(128 - inner * group, 128), 1)
            for local in range(group):
                average = here[:, local : local + 1]
                scale = here[:, half_blocks + local : half_blocks + local + 1]
                normed = (backs[g, local] - average) * scale * gain[...]
                state[g, local] = (state[g, local].astype(F32) + normed).astype(BF16)
            pltpu.make_async_copy(state.at[g], out.at[g], stores.at[g]).start()
            return 0

        lax.fori_loop(0, per_half, finish, 0)
    for g in range(groups):
        pltpu.make_async_copy(state.at[g], out.at[g], stores.at[g]).wait()
    for part in range(2):
        for j in range(1, heads):
            exchange(part, j).wait_send()


def decode(heads, table, source, weights, state, gain):
    blocks, slots, rows, _ = weights.shape
    columns = state.shape[1]
    group = 8
    groups = blocks // group
    weights = weights.reshape(groups, group, slots, rows, rows)
    shape = state.shape
    state = state.reshape(groups, group, rows, columns)
    hbm = pl.BlockSpec(memory_space=pl.ANY)
    vmem = pl.BlockSpec(memory_space=pltpu.VMEM)
    dma = pltpu.SemaphoreType.DMA
    return pl.pallas_call(
        functools.partial(decode_kernel, heads),
        out_shape=jax.ShapeDtypeStruct(state.shape, BF16),
        in_specs=[pl.BlockSpec(memory_space=pltpu.SMEM), hbm, hbm, hbm, vmem],
        out_specs=hbm,
        scratch_shapes=[
            pltpu.VMEM(source.shape, BF16),
            pltpu.VMEM(weights.shape, BF16),
            pltpu.VMEM(state.shape, BF16),
            pltpu.VMEM(state.shape, F32),
            pltpu.VMEM((2, rows, 128), F32),
            pltpu.VMEM((2, rows // 2, 128), F32),
            pltpu.VMEM((2, heads, rows // 2, 128), F32),
            dma((2 + groups,)),
            dma((groups,)),
            dma((2, heads)),
            dma((2, heads)),
        ],
        compiler_params=pltpu.CompilerParams(
            vmem_limit_bytes=63 * MIB, collective_id=2, has_side_effects=True
        ),
        cost_estimate=cost(8 * blocks * rows * rows * columns, 6 * blocks * rows * columns),
        name="decode",
    )(table, source, weights, state, gain).reshape(shape)


def on_device(
    grid_state,
    encode_index,
    encode_weights,
    first_gain,
    project_in,
    project_out,
    second_gain,
    expand_weights,
    shrink_weights,
    decode_index,
    decode_weights,
    output_gain,
):
    band_number = lax.axis_index("seq")
    band_count = lax.axis_size("seq")
    head_count = lax.axis_size("head")
    block_rows = encode_weights.shape[2]
    mesh_blocks = encode_weights.shape[0]
    mesh_rows = mesh_blocks * block_rows
    grid_blocks = grid_state.shape[0] // block_rows
    columns = grid_state.shape[1]
    heads_here = columns // HEAD_DIM
    mesh_rim = mesh_blocks // 2

    queries, keys_values, low, high, start_share, whole_out, expands, shrinks = front(
        band_count,
        head_count,
        encode_index,
        grid_state,
        encode_weights,
        first_gain.reshape(head_count, 1, columns),
        project_in.transpose(1, 0, 2),
        project_out,
        expand_weights,
        shrink_weights,
    )

    wide = middle(
        band_count,
        head_count,
        block_rows,
        queries,
        low,
        keys_values,
        high,
        start_share,
        second_gain.reshape(1, D),
        whole_out,
        expand_weights,
        shrink_weights,
        expands,
        shrinks,
    )
    return decode(
        head_count, decode_index, wide, decode_weights, grid_state, output_gain.reshape(1, columns)
    )


def solution(mesh):
    return jax.shard_map(
        on_device,
        mesh=mesh,
        in_specs=(
            P("seq", "head"),
            P("seq", None),
            P("seq", None, None, None),
            P(),
            P(None, None, "head"),
            P("head", None),
            P(),
            P(None, "head"),
            P("head", None),
            P("seq", None),
            P("seq", None, None, None),
            P("head"),
        ),
        out_specs=P("seq", "head"),
        check_vma=False,
    )
```

```python
import functools

import jax
import jax.numpy as jnp
from jax import lax
from jax.experimental import pallas as pl
from jax.experimental.pallas import tpu as pltpu
from jax.sharding import PartitionSpec as P

D = 1024
HEAD_DIM = 64
WINDOW = 1120
EPSILON = 1e-05
NEGATIVE = -1e30
LOG2_E = 1.4426950408889634
Q_TILE = 256
K_CHUNK = 512
F32 = jnp.float32
BF16 = jnp.bfloat16
MIB = 1024 * 1024
RELAY = 2
BEHIND = 3
OUT_STEP = 2
FAR_STEPS = (4, 4)
PASS_STEP = 7


def params(mib=48, dims=None):
    return pltpu.CompilerParams(vmem_limit_bytes=mib * MIB, dimension_semantics=dims)


def cost(flops, moved):
    return pl.CostEstimate(flops=int(flops), bytes_accessed=int(moved), transcendentals=0)


def reach(src, dst, send, recv, **target):
    return pltpu.make_async_remote_copy(
        src_ref=src,
        dst_ref=dst,
        send_sem=send,
        recv_sem=recv,
        device_id=target,
        device_id_type=pl.DeviceIdType.MESH,
    )


def greet(bands, heads, pair=0):
    band = lax.axis_index("seq")
    head = lax.axis_index("head")
    barrier = pltpu.get_barrier_semaphore()
    kind = pl.DeviceIdType.MESH
    for j in range(1, heads):
        pl.semaphore_signal(barrier, inc=1, device_id={"head": head ^ j}, device_id_type=kind)
    if pair:
        pl.semaphore_signal(barrier, inc=1, device_id={"seq": band ^ pair}, device_id_type=kind)

    @pl.when(band > 0)
    def _():
        pl.semaphore_signal(barrier, inc=1, device_id={"seq": band - 1}, device_id_type=kind)

    @pl.when(band < bands - 1)
    def _():
        pl.semaphore_signal(barrier, inc=1, device_id={"seq": band + 1}, device_id_type=kind)

    ends = (band > 0).astype(jnp.int32) + (band < bands - 1).astype(jnp.int32)
    pl.semaphore_wait(barrier, heads - 1 + (1 if pair else 0) + ends)


def within(number, ref):
    return jnp.clip(number, 0, ref.shape[0] - 1)


def front_kernel(bands, heads, rim_rows, *refs):
    table, state, blend, gain, project_in, project_out, expand, shrink = refs[:8]
    out_q, out_kv, out_low, out_high, out_start, out_project, out_expand, out_shrink = refs[8:16]
    wide, weights, held, projections = refs[16:20]
    loads, rim_send, rim_recv, piece_send, piece_recv, kv_send, kv_recv = refs[20:27]
    out_send, out_recv, core_send, core_recv = refs[27:31]
    gather_send, gather_recv, pair_send, pair_recv, cross_send, cross_recv = refs[31:]
    band = lax.axis_index("seq")
    head = lax.axis_index("head")
    blocks, slots, rows, _ = weights.shape
    grid_blocks, _, columns = state.shape
    mesh_rows = blocks * rows
    margin = (wide.shape[0] - grid_blocks) // 2
    chunk = 256
    chunks = mesh_rows // chunk
    base = band * grid_blocks - margin
    has_low = band > 0
    has_high = band < bands - 1
    lower = lax.max(band - 1, 0)
    upper = lax.min(band + 1, bands - 1)

    local = [
        pltpu.make_async_copy(state, wide.at[pl.ds(margin, grid_blocks)], loads.at[0]),
        pltpu.make_async_copy(blend, weights, loads.at[1]),
        pltpu.make_async_copy(project_in, projections, loads.at[2]),
        pltpu.make_async_copy(project_out, out_project.at[0], loads.at[3]),
    ]
    for copy in local:
        copy.start()
    greet(bands, heads, 2)

    down = reach(
        state.at[pl.ds(0, margin)],
        wide.at[pl.ds(margin + grid_blocks, margin)],
        rim_send.at[0],
        rim_recv.at[1],
        seq=lower,
    )
    up = reach(
        state.at[pl.ds(grid_blocks - margin, margin)],
        wide.at[pl.ds(0, margin)],
        rim_send.at[1],
        rim_recv.at[0],
        seq=upper,
    )
    pl.when(has_low)(down.start)
    pl.when(has_high)(up.start)

    relay = heads == 4
    near = range(1, 3) if relay else range(1, heads)
    cut = project_out.shape[0] // 4

    def part_rows(core, part):
        return pl.ds(pl.multiple_of((core * 2 + part) * cut, cut), cut)

    def project_part(part, owner, partner):
        here = part_rows(band % 2, part)
        source = project_out.at[here] if owner == partner else out_project.at[owner ^ partner, here]
        sems = (out_send.at[owner, part], out_recv.at[owner, part])
        return reach(source, out_project.at[owner, here], *sems, head=head ^ partner)

    def project_core(part, owner, core):
        here = out_project.at[owner, part_rows(core, part)]
        return reach(here, here, core_send.at[owner, part], core_recv.at[owner, part], seq=band ^ 1)

    half = (band // 2) % 2

    def shared_rows(array, its_core, its_half, base):
        size = (expand, shrink)[array].shape[0] // 8
        return pl.ds(pl.multiple_of((base + its_half * 2 + its_core) * size, size), size)

    def gathered(array, owner):
        table = (out_expand, out_shrink)[array]
        here = shared_rows(array, band % 2, half, 0)
        source = (expand, shrink)[array].at[shared_rows(array, band % 2, half, 4)]
        sems = (gather_send.at[owner, array], gather_recv.at[owner, array])
        return reach(source, table.at[owner, here], *sems, head=head ^ owner)

    def far(array, split):
        table = (out_expand, out_shrink)[array]
        size = (expand, shrink)[array].shape[0] // 16
        number = (half * 2 + band % 2) * 2 + split
        here = pl.ds(pl.multiple_of(number * size, size), size)
        sems = (gather_send.at[3 * split, array], gather_recv.at[3 * split, array])
        return reach(table.at[1 + split, here], table.at[3, here], *sems, head=head ^ (2 - split))

    def paired(array, owner, its_half):
        here = (out_expand, out_shrink)[array].at[owner, shared_rows(array, band % 2, its_half, 0)]
        return reach(here, here, pair_send.at[owner, array], pair_recv.at[owner, array], seq=band ^ 2)

    def crossed(array, owner, its_core, other):
        its_half = 1 - half if other else half
        here = (out_expand, out_shrink)[array].at[owner, shared_rows(array, its_core, its_half, 0)]
        at = array + 2 if other else array
        return reach(here, here, cross_send.at[owner, at], cross_recv.at[owner, at], seq=band ^ 1)

    def spread(array, owner):
        if relay and owner == 3:
            far(array, 0).wait_recv()
            far(array, 1).wait_recv()
        else:
            gathered(array, owner).wait_recv()
        crossed(array, owner, band % 2, False).start()
        paired(array, owner, half).start()

    def passed(array, owner):
        paired(array, owner, 1 - half).wait_recv()
        crossed(array, owner, band % 2, True).start()

    def advance(array):
        for j in near:
            spread(array, j)
        if relay:
            far(array, 0).start()
            far(array, 1).start()

    for array in range(2):
        for j in near:
            gathered(array, j).start()
    for part in range(2):
        for j in near:
            project_part(part, j, j).start()

    @pl.when(jnp.logical_not(has_low))
    def _():
        out_low[...] = jnp.zeros(out_low.shape, BF16)

    @pl.when(jnp.logical_not(has_high))
    def _():
        out_high[...] = jnp.zeros(out_high.shape, BF16)

    for copy in local:
        copy.wait()
    pl.when(has_low)(up.wait_recv)
    pl.when(has_high)(down.wait_recv)
    advance(0)
    advance(1)

    def place(step):
        number = jnp.where(band % 2 == 0, step, chunks - 1 - step)
        return number, pl.ds(pl.multiple_of(number * chunk, chunk), chunk)

    def piece(step, owner):
        _, here = place(step)
        return reach(
            held.at[0, here],
            held.at[owner, here],
            piece_send.at[owner, step],
            piece_recv.at[owner, step],
            head=head ^ owner,
        )

    def encode(step):
        number, _ = place(step)
        for part in range(chunk // rows):
            block = number * (chunk // rows) + part
            left = jnp.concatenate([weights[block, k] for k in range(slots)], axis=1)
            right = jnp.concatenate([wide[within(table[block, k] - base, wide)] for k in range(slots)], axis=0)
            at = pl.multiple_of(number * chunk + part * rows, rows)
            held[0, pl.ds(at, rows), :] = jnp.dot(
                left, right, preferred_element_type=F32
            ).astype(BF16)

    def project(step):
        _, here = place(step)
        values = [held[j, here, :].astype(F32) for j in range(heads)]
        average = sum(jnp.sum(v, axis=1, keepdims=True) for v in values) / D
        centred = [v - average for v in values]
        spread = sum(jnp.sum(c * c, axis=1, keepdims=True) for c in centred) / D
        scale = lax.rsqrt(spread + EPSILON)
        made = [0.0, 0.0, 0.0]
        for j in range(heads):
            owner = head ^ j
            normed = (centred[j] * scale * gain[owner]).astype(BF16)
            lines = pl.ds(pl.multiple_of(owner * columns, columns), columns)
            for t in range(3):
                made[t] += jnp.dot(normed, projections[t, lines, :], preferred_element_type=F32)
        out_q[here, :] = (made[0] * (HEAD_DIM ** (-0.5) * LOG2_E)).astype(BF16)
        out_kv[here, :columns] = made[1].astype(BF16)
        out_kv[here, columns:] = made[2].astype(BF16)

    full, rest = divmod(rim_rows, chunk)
    first = mesh_rows - rim_rows

    def rim_copies(step):
        number, here = place(step)
        start = pl.multiple_of(number * chunk, chunk)
        made = []
        whole = jnp.logical_and(has_low, number < full)
        source = out_kv.at[here]
        target = out_high.at[pl.ds(pl.multiple_of(jnp.minimum(start, (full - 1) * chunk), chunk), chunk)]
        made.append((whole, reach(source, target, kv_send.at[0, step], kv_recv.at[0, number], seq=lower)))
        whole = jnp.logical_and(has_high, number >= chunks - full)
        target = out_low.at[pl.ds(pl.multiple_of(jnp.maximum(start - first, rest), 16), chunk)]
        made.append((whole, reach(source, target, kv_send.at[1, step], kv_recv.at[1, number], seq=upper)))
        if rest:
            part = jnp.logical_and(has_low, number == full)
            source = out_kv.at[pl.ds(full * chunk, rest)]
            target = out_high.at[pl.ds(full * chunk, rest)]
            made.append((part, reach(source, target, kv_send.at[0, step], kv_recv.at[0, number], seq=lower)))
            part = jnp.logical_and(has_high, number == chunks - full - 1)
            source = out_kv.at[pl.ds(first, rest)]
            target = out_low.at[pl.ds(0, rest)]
            made.append((part, reach(source, target, kv_send.at[1, step], kv_recv.at[1, number], seq=upper)))
        return made

    def arrival(way, number, size, at):
        into = (out_high if way == 0 else out_low).at[pl.ds(at, size)]
        spare = kv_send.at[way, 0]
        return reach(into, into, spare, kv_recv.at[way, number], seq=upper if way == 0 else lower)

    def diagonal(step, split):
        number, _ = place(step)
        size = chunk // 2
        here = pl.ds(pl.multiple_of(number * chunk + split * size, size), size)
        sems = (piece_send.at[3 * split, step], piece_recv.at[3 * split, step])
        return reach(held.at[1 + split, here], held.at[3, here], *sems, head=head ^ (2 - split))

    for step in range(chunks + BEHIND):
        if step < chunks:
            encode(step)
            for j in (range(1, 3) if relay else range(1, heads)):
                piece(step, j).start()
        old = step - RELAY
        if relay and 0 <= old < chunks:
            for split in range(2):
                piece(old, 1 + split).wait_recv()
                diagonal(old, split).start()
        old = step - BEHIND
        if old >= 0:
            if relay:
                diagonal(old, 0).wait_recv()
                diagonal(old, 1).wait_recv()
            else:
                for j in range(1, heads):
                    piece(old, j).wait_recv()
            project(old)
            for here, copy in rim_copies(old):
                pl.when(here)(copy.start)
        if step == OUT_STEP:
            for part in range(2):
                for j in near:
                    project_part(part, j, j).wait_recv()
                if relay:
                    project_part(part, 3, 2 - part).start()
                for j in near:
                    project_core(part, j, band % 2).start()
        if relay and step in FAR_STEPS:
            spread(0, 3)
            spread(1, 3)
        if step == PASS_STEP:
            for array in range(2):
                for j in near:
                    passed(array, j)

    for array in range(2):
        if relay:
            passed(array, 3)
    for array in range(2):
        for j in range(1, heads):
            crossed(array, j, 1 - band % 2, False).wait_recv()
            crossed(array, j, 1 - band % 2, True).wait_recv()
            crossed(array, j, band % 2, False).wait_send()
            crossed(array, j, band % 2, True).wait_send()
            paired(array, j, half).wait_send()
            if j in near:
                gathered(array, j).wait_send()
        if relay:
            far(array, 0).wait_send()
            far(array, 1).wait_send()
    for part in range(2):
        if relay:
            project_part(part, 3, 2 - part).wait()
            project_core(part, 3, band % 2).start()
        for j in near:
            project_part(part, j, j).wait_send()
    for part in range(2):
        for j in range(1, heads):
            project_core(part, j, band % 2).wait_send()
            project_core(part, j, 1 - band % 2).wait_recv()

    share = out_start.shape[1]
    mine = pl.ds(pl.multiple_of(head * share, share), share)
    for j in range(heads):
        out_start[head ^ j] = held[j, mine, :]

    pl.when(has_low)(down.wait_send)
    pl.when(has_high)(up.wait_send)
    for step in range(chunks):
        for j in (range(1, 3) if relay else range(1, heads)):
            piece(step, j).wait_send()
        if relay:
            diagonal(step, 0).wait_send()
            diagonal(step, 1).wait_send()
        for here, copy in rim_copies(step):
            pl.when(here)(copy.wait_send)

    for number in range(full):
        pl.when(has_high)(arrival(0, number, chunk, number * chunk).wait_recv)
        other = chunks - full + number
        pl.when(has_low)(arrival(1, other, chunk, rest + number * chunk).wait_recv)
    if rest:
        pl.when(has_high)(arrival(0, full, rest, full * chunk).wait_recv)
        pl.when(has_low)(arrival(1, chunks - full - 1, rest, 0).wait_recv)


def front(bands, heads, table, state, blend, gain, *others):
    project_in, project_out, expand, shrink = others
    blocks, slots, rows, _ = blend.shape
    grid_rows, columns = state.shape
    grid_blocks = grid_rows // rows
    state = state.reshape(grid_blocks, rows, columns)
    mesh_rows = blocks * rows
    rim_rows = min(mesh_rows, WINDOW)
    chunks = mesh_rows // 256
    vmem = pl.BlockSpec(memory_space=pltpu.VMEM)
    hbm = pl.BlockSpec(memory_space=pl.ANY)
    shape = lambda *sizes: jax.ShapeDtypeStruct(sizes, BF16)
    dma = pltpu.SemaphoreType.DMA
    return pl.pallas_call(
        functools.partial(front_kernel, bands, heads, rim_rows),
        out_shape=[
            shape(mesh_rows, columns),
            shape(mesh_rows, 2 * columns),
            shape(rim_rows, 2 * columns),
            shape(rim_rows, 2 * columns),
            shape(heads, mesh_rows // heads, columns),
            shape(heads, *project_out.shape),
            shape(heads, expand.shape[0] // 2, expand.shape[1]),
            shape(heads, shrink.shape[0] // 2, shrink.shape[1]),
        ],
        in_specs=[pl.BlockSpec(memory_space=pltpu.SMEM), hbm, hbm, vmem] + [hbm] * 4,
        out_specs=[vmem] * 6 + [hbm] * 2,
        scratch_shapes=[
            pltpu.VMEM((grid_blocks + 2 * blocks, rows, columns), BF16),
            pltpu.VMEM(blend.shape, BF16),
            pltpu.VMEM((heads, mesh_rows, columns), BF16),
            pltpu.VMEM(project_in.shape, BF16),
            dma((4,)),
            dma((2,)),
            dma((2,)),
            dma((heads, chunks)),
            dma((heads, chunks)),
            dma((2, chunks)),
            dma((2, chunks)),
            *[dma((heads, 2))] * 8,
            *[dma((heads, 4))] * 2,
        ],
        compiler_params=pltpu.CompilerParams(
            vmem_limit_bytes=60 * MIB, collective_id=0, has_side_effects=True
        ),
        cost_estimate=cost(6 * mesh_rows * D * columns * 20, grid_rows * columns * 4),
        name="front",
    )(table, state, blend, gain, *others)


def middle_kernel(bands, heads, *refs):
    queries, low, own, high, begun, gain, project_out, expand, shrink, half_e, half_s = refs[:11]
    wide = refs[11]
    keys, values, scores, masks, sent, context = refs[12:18]
    expands, shrinks, total, normed, finished, loads = refs[18:24]
    context_send, context_recv, gather_send, gather_recv, core_send, core_recv = refs[24:30]
    pair_send, pair_recv, end_send, end_recv, rim_send, rim_recv = refs[30:]
    band = lax.axis_index("seq")
    head = lax.axis_index("head")
    core, half = band % 2, (band // 2) % 2
    lower = lax.max(band - 1, 0)
    upper = lax.min(band + 1, bands - 1)
    has_low = band > 0
    has_high = band < bands - 1
    rows, columns = queries.shape
    rim = low.shape[0]
    count = columns // HEAD_DIM
    width = scores.shape[2]
    chunks = width // K_CHUNK
    tiles = rows // Q_TILE
    share = rows // heads
    per_share = share // Q_TILE
    units = expand.shape[1]
    relay = heads == 4
    near = range(1, 3) if relay else range(1, heads)

    greet(bands, heads, 2)

    parts = [(1, 2), (0, 0), (0, 1)]

    def part_rows(part, its_core, its_half, split=None):
        array, kind = parts[part]
        size = (expand if array == 0 else shrink).shape[0] // 8
        number = (its_half if kind == 2 else kind) + its_core * 2
        at = number * size
        if split is not None:
            size //= 2
            at += split * size
        return (expands, shrinks)[array], pl.ds(pl.multiple_of(at, size), size)

    def gathered(part, owner):
        table, here = part_rows(part, core, half)
        source = (expand if parts[part][0] == 0 else shrink).at[here]
        sems = (gather_send.at[owner, part], gather_recv.at[owner, part])
        return reach(source, table.at[owner, here], *sems, head=head ^ owner)

    def far(part, split):
        table, here = part_rows(part, core, half, split)
        sems = (gather_send.at[3 * split, part], gather_recv.at[3 * split, part])
        return reach(table.at[1 + split, here], table.at[3, here], *sems, head=head ^ (2 - split))

    def paired(part, owner, its_half):
        table, here = part_rows(part, core, its_half)
        here = table.at[owner, here]
        return reach(here, here, pair_send.at[owner], pair_recv.at[owner], seq=band ^ 2)

    def crossed(part, owner, its_core, other=False):
        table, here = part_rows(part, its_core, 1 - half if other else half)
        here, at = table.at[owner, here], len(parts) if other else part
        return reach(here, here, core_send.at[owner, at], core_recv.at[owner, at], seq=band ^ 1)

    def spread(part, owner):
        if relay and owner == 3:
            far(part, 0).wait_recv()
            far(part, 1).wait_recv()
        else:
            gathered(part, owner).wait_recv()
        if part == 0:
            paired(part, owner, half).start()
        crossed(part, owner, core).start()

    def passed(owner):
        paired(0, owner, 1 - half).wait_recv()
        crossed(0, owner, core, True).start()

    def advance(part):
        for j in near:
            spread(part, j)
        if relay:
            far(part, 0).start()
            far(part, 1).start()

    def begin(part):
        for j in near:
            gathered(part, j).start()

    def arrived(owner):
        for part in range(len(parts)):
            crossed(part, owner, 1 - core).wait_recv()
        crossed(0, owner, 1 - core, True).wait_recv()

    begin(0)
    begin(1)
    local = [
        pltpu.make_async_copy(expand, expands.at[0], loads.at[0]),
        pltpu.make_async_copy(shrink, shrinks.at[0], loads.at[1]),
    ]
    for j in range(1, heads):
        for array, (given, table) in enumerate(((half_e, expands), (half_s, shrinks))):
            size = given.shape[1]
            local.append(
                pltpu.make_async_copy(given.at[j], table.at[j, pl.ds(size, size)], loads.at[2 * j + array])
            )
    for copy in local:
        copy.start()

    lane = lax.broadcasted_iota(jnp.int32, (1, 128), 1)
    for h in range(count):
        lanes = slice(128 * (h // 2), 128 * (h // 2 + 1))
        value_lanes = slice(columns + 128 * (h // 2), columns + 128 * (h // 2 + 1))
        is_mine = (lane < HEAD_DIM) if h % 2 == 0 else (lane >= HEAD_DIM)
        marker = lane == (HEAD_DIM if h % 2 == 0 else 0)
        at = 0
        for source in (low, own, high):
            size = source.shape[0]
            number = band * rows - rim + at + lax.broadcasted_iota(jnp.int32, (size, 1), 0)
            outside = jnp.logical_or(number < 0, number >= bands * rows)
            mark = jnp.where(jnp.logical_and(outside, marker), NEGATIVE, 0.0).astype(BF16)
            keys[h, at : at + size, :] = jnp.where(is_mine, source[:, lanes], mark)
            found = source[:, value_lanes]
            values[h, at : at + size, :] = jnp.where(is_mine, found, jnp.ones_like(found))
            at += size
        end = keys.shape[1] - at
        if end:
            keys[h, at:, :] = jnp.zeros((end, 128), BF16)
            values[h, at:, :] = jnp.zeros((end, 128), BF16)
    q_iota = lax.broadcasted_iota(jnp.int32, (Q_TILE, K_CHUNK), 0)
    k_iota = lax.broadcasted_iota(jnp.int32, (Q_TILE, K_CHUNK), 1)
    for n, c in enumerate((0, chunks - 1)):
        distance = k_iota + c * K_CHUNK - q_iota
        allowed = (distance >= 0) & (distance <= 2 * WINDOW)
        masks[n] = jnp.where(allowed, 0.0, NEGATIVE)

    def where_at(step):
        partner = head ^ (heads - 1 - step // per_share)
        tile = partner * per_share + step % per_share
        return pl.multiple_of(tile * Q_TILE, Q_TILE)

    def context_copy(step):
        mask = heads - 1 - step // per_share
        at = pl.ds(pl.multiple_of((step % per_share) * Q_TILE, Q_TILE), Q_TILE)
        sems = (context_send.at[step], context_recv.at[step])
        return reach(sent.at[step], context.at[head, at], *sems, head=head ^ mask)

    def query_of(start, h):
        pair = queries[pl.ds(start, Q_TILE), 128 * (h // 2) : 128 * (h // 2 + 1)]
        is_key = (lane < HEAD_DIM) if h % 2 == 0 else (lane >= HEAD_DIM)
        marker = lane == (HEAD_DIM if h % 2 == 0 else 0)
        return jnp.where(is_key, pair, jnp.where(marker, 1.0, 0.0).astype(BF16))

    def score_chunk(start, h, query, peak, c):
        key = keys[h, pl.ds(start + c * K_CHUNK, K_CHUNK), :]
        score = lax.dot_general(query, key, (((1,), (1,)), ((), ())), preferred_element_type=F32)
        if c == 0:
            score += masks[0]
        if c == chunks - 1:
            score += masks[1]
        scores[h % 2, :, c * K_CHUNK : (c + 1) * K_CHUNK] = score
        for part in range(K_CHUNK // 128):
            piece = score[:, part * 128 : (part + 1) * 128]
            peak = piece if peak is None else jnp.maximum(peak, piece)
        return peak

    def attend(step, _):
        start = where_at(step)
        outs = []
        peak = None
        query = query_of(start, 0)
        for c in range(chunks):
            peak = score_chunk(start, 0, query, peak, c)
        for h in range(count):
            top = jnp.max(peak, axis=1, keepdims=True)
            found, peak = 0.0, None
            if h + 1 < count:
                query = query_of(start, h + 1)
            for c in range(chunks):
                if h + 1 < count:
                    peak = score_chunk(start, h + 1, query, peak, c)
                power = jnp.exp2(scores[h % 2, :, c * K_CHUNK : (c + 1) * K_CHUNK] - top)
                value = values[h, pl.ds(start + c * K_CHUNK, K_CHUNK), :]
                found += jnp.dot(power.astype(BF16), value, preferred_element_type=F32)
            weight = pltpu.roll(found, HEAD_DIM, 1)
            outs.append(found / weight)
        for g in range(count // 2):
            first, second = outs[2 * g], outs[2 * g + 1]
            both = jnp.where(lane < HEAD_DIM, first, second)
            sent[step, :, 128 * g : 128 * (g + 1)] = both.astype(BF16)

        @pl.when(step < (heads - 1) * per_share)
        def _():
            context_copy(step).start()

        @pl.when(step == (heads - 1) * per_share)
        def _():
            begin(2)
            advance(0)
            advance(1)

        return 0

    lax.fori_loop(0, tiles, attend, 0)
    for step in range((heads - 1) * per_share, tiles):
        at = (step % per_share) * Q_TILE
        context[head, at : at + Q_TILE, :] = sent[step]
    for step in range((heads - 1) * per_share):
        context_copy(step).wait_recv()

    attended = 0.0
    for j in range(heads):
        attended += jnp.dot(context[head ^ j], project_out[j], preferred_element_type=F32)
    start = jnp.concatenate([begun[j] for j in range(heads)], axis=1)
    middle = (start.astype(F32) + attended).astype(BF16).astype(F32)
    total[...] = middle
    average = jnp.mean(middle, axis=1, keepdims=True)
    centred = middle - average
    spread_of = jnp.mean(centred * centred, axis=1, keepdims=True)
    normed[...] = (centred * lax.rsqrt(spread_of + EPSILON) * gain[...]).astype(BF16)
    for copy in local:
        copy.wait()

    def feed(j, here):
        piece = units // 2
        for n in range(2):
            lanes = slice(n * piece, (n + 1) * piece)
            tall = jnp.dot(normed[here, :], expands[j, :, lanes], preferred_element_type=F32)
            hidden = jax.nn.gelu(tall).astype(BF16)
            total[here, :] += jnp.dot(hidden, shrinks[j, lanes, :], preferred_element_type=F32)

    advance(2)
    feed(0, slice(0, share))
    for j in near:
        passed(j)
    if relay:
        spread(0, 3)
    for j in range(1, heads):
        if relay and j == 2:
            spread(1, 3)
        if relay and j == 3:
            spread(2, 3)
            passed(3)
        arrived(j)
        if j < heads - 1:
            feed(j, slice(0, share))

    blocks, block_rows = wide.shape[0] // 2, wide.shape[1]
    edge = blocks // 2
    part_blocks = finished.shape[2]
    halves = finished.shape[1]

    def end_block(owner, number):
        return owner * halves * part_blocks + number * part_blocks

    def end_copy(mask, number):
        at = pl.ds(edge + end_block(head, number), part_blocks)
        sems = (end_send.at[mask, number], end_recv.at[mask, number])
        return reach(finished.at[head ^ mask, number], wide.at[at], *sems, head=head ^ mask)

    def rim_copies(mask, number):
        block = end_block(head ^ mask, number)
        here = wide.at[pl.ds(edge + block, part_blocks)]
        below = wide.at[pl.ds(edge + blocks + jnp.minimum(block, edge - part_blocks), part_blocks)]
        above_block = jnp.maximum(block - (blocks - edge), 0)
        above = wide.at[pl.ds(above_block, part_blocks)]
        sem = rim_send.at[mask, number]
        down_sem = rim_recv.at[0, jnp.minimum(block, edge - part_blocks) // part_blocks]
        up_sem = rim_recv.at[1, above_block // part_blocks]
        return [
            (jnp.logical_and(has_low, block < edge), reach(here, below, sem, down_sem, seq=lower)),
            (jnp.logical_and(has_high, block >= blocks - edge), reach(here, above, sem, up_sem, seq=upper)),
        ]

    size = share // halves
    for number in range(halves):
        here = slice(number * size, (number + 1) * size)
        feed(heads - 1, here)
        for j in range(heads):
            lanes = slice(j * columns, (j + 1) * columns)
            piece = total[here, lanes].astype(BF16).reshape(part_blocks, block_rows, columns)
            finished[j, number] = piece
        for j in range(heads - 1, 0, -1):
            end_copy(j, number).start()
        wide[pl.ds(edge + end_block(head, number), part_blocks)] = finished[head, number]
        for here, copy in rim_copies(0, number):
            pl.when(here)(copy.start)
    for number in range(halves):
        for j in range(1, heads):
            end_copy(j, number).wait_recv()
            for here, copy in rim_copies(j, number):
                pl.when(here)(copy.start)
    for number in range(edge // part_blocks):
        below = wide.at[pl.ds(edge + blocks + number * part_blocks, part_blocks)]
        above = wide.at[pl.ds(number * part_blocks, part_blocks)]
        spare = rim_send.at[0, 0]
        pl.when(has_high)(reach(below, below, spare, rim_recv.at[0, number], seq=upper).wait_recv)
        pl.when(has_low)(reach(above, above, spare, rim_recv.at[1, number], seq=lower).wait_recv)

    for step in range((heads - 1) * per_share):
        context_copy(step).wait_send()
    for part in range(len(parts)):
        for j in near:
            gathered(part, j).wait_send()
        if relay:
            far(part, 0).wait_send()
            far(part, 1).wait_send()
        for j in range(1, heads):
            crossed(part, j, core).wait_send()
    for j in range(1, heads):
        paired(0, j, half).wait_send()
        crossed(0, j, core, True).wait_send()
    for number in range(halves):
        for j in range(heads):
            if j:
                end_copy(j, number).wait_send()
            for here, copy in rim_copies(j, number):
                pl.when(here)(copy.wait_send)


def middle(bands, heads, block_rows, queries, *others):
    expand = others[6]
    rows, columns = queries.shape
    share = rows // heads
    depth, units = expand.shape
    count = columns // HEAD_DIM
    width = -(-(Q_TILE + 2 * WINDOW) // K_CHUNK) * K_CHUNK
    wide_rows = rows - Q_TILE + width
    tiles = rows // Q_TILE
    halves = 2 if share >= 4 * block_rows else 1
    part_blocks = share // halves // block_rows
    blocks = rows // block_rows
    vmem = pl.BlockSpec(memory_space=pltpu.VMEM)
    hbm = pl.BlockSpec(memory_space=pl.ANY)
    dma = pltpu.SemaphoreType.DMA
    return pl.pallas_call(
        functools.partial(middle_kernel, bands, heads),
        out_shape=jax.ShapeDtypeStruct((2 * blocks, block_rows, columns), BF16),
        in_specs=[vmem] * 7 + [hbm] * 4,
        out_specs=vmem,
        scratch_shapes=[
            pltpu.VMEM((count, wide_rows, 128), BF16),
            pltpu.VMEM((count, wide_rows, 128), BF16),
            pltpu.VMEM((2, Q_TILE, width), F32),
            pltpu.VMEM((2, Q_TILE, K_CHUNK), F32),
            pltpu.VMEM((tiles, Q_TILE, columns), BF16),
            pltpu.VMEM((heads, share, columns), BF16),
            pltpu.VMEM((heads, depth, units), BF16),
            pltpu.VMEM((heads, units, depth), BF16),
            pltpu.VMEM((share, depth), F32),
            pltpu.VMEM((share, depth), BF16),
            pltpu.VMEM((heads, halves, part_blocks, block_rows, columns), BF16),
            dma((2 * heads,)),
            dma((tiles,)),
            dma((tiles,)),
            *[dma((heads, 4))] * 4,
            *[dma((heads,))] * 2,
            dma((heads, halves)),
            dma((heads, halves)),
            dma((heads, halves)),
            dma((2, blocks // 2 // part_blocks)),
        ],
        compiler_params=pltpu.CompilerParams(
            vmem_limit_bytes=63 * MIB, collective_id=1, has_side_effects=True
        ),
        cost_estimate=cost(40 * rows * width * columns, rows * columns * 8),
        name="middle",
    )(queries, *others)


def decode_kernel(heads, *refs):
    table, source, weights_in, state_in, gain, out = refs[:6]
    wide, weights, state, backs, sums, packed, theirs, loads, stores, send, recv = refs[6:]
    head = lax.axis_index("head")
    barrier = pltpu.get_barrier_semaphore()
    groups, group, rows, columns = backs.shape
    slots = weights.shape[2]
    per_half = groups // 2
    half_blocks = per_half * group
    edge = wide.shape[0] // 4
    base = lax.axis_index("seq") * 2 * edge - edge

    loads_of = [pltpu.make_async_copy(source, wide, loads.at[0])]
    for g in range(groups):
        loads_of.append(pltpu.make_async_copy(weights_in.at[g], weights.at[g], loads.at[1 + g]))
    state_load = pltpu.make_async_copy(state_in, state, loads.at[1 + groups])
    for copy in loads_of:
        copy.start()
    state_load.start()
    for j in range(1, heads):
        pl.semaphore_signal(
            barrier, inc=1, device_id={"head": head ^ j}, device_id_type=pl.DeviceIdType.MESH
        )
    pl.semaphore_wait(barrier, heads - 1)

    def exchange(part, j):
        sems = (send.at[part, j], recv.at[part, j])
        return reach(packed.at[part], theirs.at[part, j], *sems, head=head ^ j)

    lane = lax.broadcasted_iota(jnp.int32, (rows, 128), 1)
    loads_of[0].wait()
    sums[...] = jnp.zeros(sums.shape, F32)
    for part in range(2):

        def gather(inner, _):
            g = part * per_half + inner
            pltpu.make_async_copy(weights_in.at[g], weights.at[g], loads.at[1 + g]).wait()
            found = sums[part]
            for local in range(group):
                block = g * group + local
                left = jnp.concatenate([weights[g, local, k] for k in range(slots)], axis=1)
                right = jnp.concatenate([wide[within(table[block, k] - base, wide)] for k in range(slots)], axis=0)
                back = jnp.dot(left, right, preferred_element_type=F32)
                backs[g, local] = back
                once = jnp.sum(back, axis=1, keepdims=True)
                twice = jnp.sum(back * back, axis=1, keepdims=True)
                at = inner * group + local
                found = jnp.where(lane == at, once, found)
                found = jnp.where(lane == at + half_blocks, twice, found)
            sums[part] = found
            return 0

        lax.fori_loop(0, per_half, gather, 0)
        found = sums[part]
        lower = pltpu.roll(found[rows // 2 :], 64, 1)
        packed[part] = jnp.where(lane[: rows // 2] < 64, found[: rows // 2], lower)
        for j in range(1, heads):
            exchange(part, j).start()

    state_load.wait()
    for part in range(2):
        for j in range(1, heads):
            exchange(part, j).wait_recv()
        whole = packed[part]
        for j in range(1, heads):
            whole = whole + theirs[part, j]
        whole = jnp.concatenate([whole, pltpu.roll(whole, 64, 1)], axis=0) / D
        squares = pltpu.roll(whole, 128 - half_blocks, 1)
        sums[part] = jnp.where(lane < half_blocks, whole, 0.0)
        scale = lax.rsqrt(squares - whole * whole + EPSILON)
        scale = pltpu.roll(jnp.where(lane < half_blocks, scale, 0.0), half_blocks, 1)
        sums[part] = jnp.where(lane < half_blocks, whole, scale)

        def finish(inner, _):
            g = part * per_half + inner
            here = pltpu.roll(sums[part], lax.rem(128 - inner * group, 128), 1)
            for local in range(group):
                average = here[:, local : local + 1]
                scale = here[:, half_blocks + local : half_blocks + local + 1]
                normed = (backs[g, local] - average) * scale * gain[...]
                state[g, local] = (state[g, local].astype(F32) + normed).astype(BF16)
            pltpu.make_async_copy(state.at[g], out.at[g], stores.at[g]).start()
            return 0

        lax.fori_loop(0, per_half, finish, 0)
    for g in range(groups):
        pltpu.make_async_copy(state.at[g], out.at[g], stores.at[g]).wait()
    for part in range(2):
        for j in range(1, heads):
            exchange(part, j).wait_send()


def decode(heads, table, source, weights, state, gain):
    blocks, slots, rows, _ = weights.shape
    columns = state.shape[1]
    group = 8
    groups = blocks // group
    weights = weights.reshape(groups, group, slots, rows, rows)
    shape = state.shape
    state = state.reshape(groups, group, rows, columns)
    hbm = pl.BlockSpec(memory_space=pl.ANY)
    vmem = pl.BlockSpec(memory_space=pltpu.VMEM)
    dma = pltpu.SemaphoreType.DMA
    return pl.pallas_call(
        functools.partial(decode_kernel, heads),
        out_shape=jax.ShapeDtypeStruct(state.shape, BF16),
        in_specs=[pl.BlockSpec(memory_space=pltpu.SMEM), hbm, hbm, hbm, vmem],
        out_specs=hbm,
        scratch_shapes=[
            pltpu.VMEM(source.shape, BF16),
            pltpu.VMEM(weights.shape, BF16),
            pltpu.VMEM(state.shape, BF16),
            pltpu.VMEM(state.shape, F32),
            pltpu.VMEM((2, rows, 128), F32),
            pltpu.VMEM((2, rows // 2, 128), F32),
            pltpu.VMEM((2, heads, rows // 2, 128), F32),
            dma((2 + groups,)),
            dma((groups,)),
            dma((2, heads)),
            dma((2, heads)),
        ],
        compiler_params=pltpu.CompilerParams(
            vmem_limit_bytes=63 * MIB, collective_id=2, has_side_effects=True
        ),
        cost_estimate=cost(8 * blocks * rows * rows * columns, 6 * blocks * rows * columns),
        name="decode",
    )(table, source, weights, state, gain).reshape(shape)


def on_device(
    grid_state,
    encode_index,
    encode_weights,
    first_gain,
    project_in,
    project_out,
    second_gain,
    expand_weights,
    shrink_weights,
    decode_index,
    decode_weights,
    output_gain,
):
    band_number = lax.axis_index("seq")
    band_count = lax.axis_size("seq")
    head_count = lax.axis_size("head")
    block_rows = encode_weights.shape[2]
    mesh_blocks = encode_weights.shape[0]
    mesh_rows = mesh_blocks * block_rows
    grid_blocks = grid_state.shape[0] // block_rows
    columns = grid_state.shape[1]
    heads_here = columns // HEAD_DIM
    mesh_rim = mesh_blocks // 2

    queries, keys_values, low, high, start_share, whole_out, expands, shrinks = front(
        band_count,
        head_count,
        encode_index,
        grid_state,
        encode_weights,
        first_gain.reshape(head_count, 1, columns),
        project_in.transpose(1, 0, 2),
        project_out,
        expand_weights,
        shrink_weights,
    )

    wide = middle(
        band_count,
        head_count,
        block_rows,
        queries,
        low,
        keys_values,
        high,
        start_share,
        second_gain.reshape(1, D),
        whole_out,
        expand_weights,
        shrink_weights,
        expands,
        shrinks,
    )
    return decode(
        head_count, decode_index, wide, decode_weights, grid_state, output_gain.reshape(1, columns)
    )


def solution(mesh):
    return jax.shard_map(
        on_device,
        mesh=mesh,
        in_specs=(
            P("seq", "head"),
            P("seq", None),
            P("seq", None, None, None),
            P(),
            P(None, None, "head"),
            P("head", None),
            P(),
            P(None, "head"),
            P("head", None),
            P("seq", None),
            P("seq", None, None, None),
            P("head"),
        ),
        out_specs=P("seq", "head"),
        check_vma=False,
    )
```
